32 devices in a mesh: grp: 4 (over z), dev: 8 (over y, x, core).
Axes of the slice: x: 2, y: 2, z: 4, core: 2. Of those that a mesh axis runs over, the one named last changes fastest.
Arguments:
- a_blocks: bfloat16 [1024, 7, 192, 192], P(('grp', 'dev')), may hold values from -0.4375 to 0.4375
- prolong_t: bfloat16 [1024, 32, 192], P(('grp', 'dev')), may hold values from -1.796875 to 1.796875
- elem_slot: int32 [1024], P(('grp', 'dev')), may hold values from 0 to 5, as said below
- touch_agg: int32 [32, 6], replicated, may hold values from 0 to 135, as said below
- nbr: int32 [1024, 6], P(('grp', 'dev')), may hold values from -1 to 1023, as said below
- nbr_agg: int32 [1024, 6], P(('grp', 'dev')), may hold values from -1 to 135, as said below
- coarse_row: int32 [136], replicated, may hold values from 0 to 191, as said below
Outputs:
- coarse: float32 [192, 7, 1024], P('dev')
The draws below stay inside these ranges and needn't reach their ends.
Inputs may be any that keep to these rules, and one draw needn't show every extreme that they name: Element e lies on device e // 32 (devices numbered grp-major). elem_slot[e] is the position of e's aggregate in touch_agg[e // 32]. `touch_agg`: each row lists 6 distinct aggregates, exactly those of the device's elements; all devices that touch one aggregate share their grp index. `nbr`: global element index across each face, or -1 on the domain's boundary; adjacency is symmetric; a neighbour lies on the same device, or on the device whose grp index differs by one (same dev index), or whose dev index differs by one (same grp index); exactly 8 elements of a device have a neighbour on each existing device next along grp, and exactly 8 on each existing device next along dev. `nbr_agg`: the aggregate of the element nbr[e, f], -1 exactly where nbr[e, f] is -1. Distinct values; aggregate a's row belongs to dev index coarse_row[a] // 24. Of the aggregates touched by one device at most 1 belong to one dev index, and of those touched by the devices of one grp index at most 6; one dev index reaches both bounds and holds 24 rows.
All inputs are finite; a program needn't handle non-finite values.
Results may differ from the reference program's by a relative error of at most 0.005.
Values may be sent and summed in bfloat16 or wider, within the bound.
A program may use at most 128 MiB of HBM per device.

```python
import jax
import jax.numpy as jnp
from jax import lax

B = 192
C = 32
EX = 4
EY = 4
EZ = 2
E_DEV = 32
ELEMS = 1024
TOUCH = 6
SEND_CAP = 1
NYBOX = 17
AGG = 136
ROWS_OWN = 24
COARSE = 192
N_GRP = 4
N_DEV = 8


def face_fields(field):
    padded = jnp.pad(field, 1, constant_values=-1)
    return jnp.stack([padded[:-2, 1:-1, 1:-1], padded[2:, 1:-1, 1:-1], padded[1:-1, :-2, 1:-1], padded[1:-1, 2:, 1:-1], padded[1:-1, 1:-1, :-2], padded[1:-1, 1:-1, 2:]], axis=-1)


def geometry(key):
    keys = jax.random.split(jax.random.fold_in(key, 11), 6)
    devices = N_GRP * N_DEV
    half_x = EX // 2
    half_y = EY // 2
    span_y = half_y + 1
    half_z = EZ // 2
    coord_x, coord_y, coord_z = jnp.meshgrid(jnp.arange(N_GRP * EX, dtype=jnp.int32), jnp.arange(N_DEV * EY, dtype=jnp.int32), jnp.arange(EZ, dtype=jnp.int32), indexing='ij')
    grp_of = coord_x // EX
    dev_of = coord_y // EY
    device = grp_of * N_DEV + dev_of
    canon = (coord_x % EX * EY + coord_y % EY) * EZ + coord_z
    local_perms = jax.vmap(lambda k: jax.random.permutation(k, E_DEV))(jax.random.split(keys[0], devices))
    global_id = (device * E_DEV + local_perms[device, canon]).astype(jnp.int32)
    box_x = coord_x // 2
    box_y = (coord_y + 1) // 2
    box_z = coord_z // 2
    box = (box_x * NYBOX + box_y) * half_z + box_z
    box_perm = jax.random.permutation(keys[1], AGG).astype(jnp.int32)
    agg = box_perm[box]
    canon_touch = ((box_x - grp_of * half_x) * span_y + (box_y - dev_of * half_y)) * half_z + box_z
    touch_perms = jax.vmap(lambda k: jax.random.permutation(k, TOUCH))(jax.random.split(keys[2], devices))
    slot = touch_perms[device, canon_touch].astype(jnp.int32)
    touch = jnp.zeros((devices, TOUCH), jnp.int32).at[device, slot].set(agg)
    classes = jnp.arange(TOUCH, dtype=jnp.int32)
    class_ry = classes // half_z % span_y
    shuffled = jax.random.permutation(keys[3], TOUCH).astype(jnp.int32)
    score = jnp.where(class_ry != 0, TOUCH, 0) + shuffled
    order = jnp.argsort(score, stable=True)
    class_rank = jnp.zeros((TOUCH,), jnp.int32).at[order].set(classes)
    owner_perm = jax.random.permutation(keys[4], N_DEV).astype(jnp.int32)
    owner_class = jnp.where(class_rank < SEND_CAP, owner_perm[0], owner_perm[1 + (class_rank - SEND_CAP) % (N_DEV - 1)])
    grid_x, grid_y, grid_z = jnp.meshgrid(jnp.arange(N_GRP * half_x, dtype=jnp.int32), jnp.arange(NYBOX, dtype=jnp.int32), jnp.arange(half_z, dtype=jnp.int32), indexing='ij')
    class_box = ((grid_x % half_x * span_y + grid_y % span_y) * half_z + grid_z).reshape(-1)
    owner_box = owner_class[class_box]
    priority = jax.random.permutation(keys[5], AGG).astype(jnp.int32)
    earlier = (owner_box[None, :] == owner_box[:, None]) & (priority[None, :] < priority[:, None])
    position = jnp.sum(earlier.astype(jnp.int32), axis=1)
    row_box = (owner_box * ROWS_OWN + position).astype(jnp.int32)
    coarse_rows = jnp.zeros((AGG,), jnp.int32).at[box_perm].set(row_box)
    flat_ids = global_id.reshape(-1)
    elem_slots = jnp.zeros((ELEMS,), jnp.int32).at[flat_ids].set(slot.reshape(-1))
    neighbours = jnp.zeros((ELEMS, 6), jnp.int32).at[flat_ids].set(face_fields(global_id).reshape(-1, 6))
    neighbour_aggs = jnp.zeros((ELEMS, 6), jnp.int32).at[flat_ids].set(face_fields(agg).reshape(-1, 6))
    return (elem_slots, touch, neighbours, neighbour_aggs, coarse_rows)


def draw_elem_slot(key, part):
    return geometry(key)[0]


def draw_touch_agg(key, part):
    return geometry(key)[1]


def draw_nbr(key, part):
    return geometry(key)[2]


def draw_nbr_agg(key, part):
    return geometry(key)[3]


def draw_coarse_row(key, part):
    return geometry(key)[4]


def level_of(rng, shape, cuts, smallest, top_value):
    gain, own = 1.0, jax.random.fold_in(rng, 6)
    for axis_at, blocks in cuts:
        steps = jnp.exp(jax.random.uniform(jax.random.fold_in(own, axis_at), (blocks,), jnp.float32, smallest / len(cuts), top_value / len(cuts)))
        gain = gain * jnp.repeat(steps, shape[axis_at] // blocks).reshape([-1 if axis == axis_at else 1 for axis in range(len(shape))])
    return gain


def centred(stream_key, dims, scale, bound, shards=(), kind=jnp.bfloat16):
    result = jax.random.normal(stream_key, dims, jnp.float32) * scale
    if len(shards) > 0:
        result = level_of(stream_key, dims, shards, -0.22, 0.18) * result
    return jnp.clip(result, min=-bound, max=bound).astype(kind)


def setup_inputs(seed: int = 0) -> dict:
    streams_of = jax.random.split(jax.random.key(seed), 8)
    a_blocks = centred(streams_of[0], (ELEMS, 7, B, B), B ** -0.5, 0.4375, ((0, 32),))
    prolong_t = centred(streams_of[1], (ELEMS, C, B), 0.3, 1.796875, ((0, 32),))
    elem_slot = draw_elem_slot(jax.random.fold_in(streams_of[7], 71), 0)
    touch_agg = draw_touch_agg(jax.random.fold_in(streams_of[7], 71), 0)
    nbr = draw_nbr(jax.random.fold_in(streams_of[7], 71), 0)
    nbr_agg = draw_nbr_agg(jax.random.fold_in(streams_of[7], 71), 0)
    coarse_row = draw_coarse_row(jax.random.fold_in(streams_of[7], 71), 0)
    return dict(a_blocks=a_blocks, prolong_t=prolong_t, elem_slot=elem_slot, touch_agg=touch_agg, nbr=nbr, nbr_agg=nbr_agg, coarse_row=coarse_row)


def reference(a_blocks, prolong_t, elem_slot, touch_agg, nbr, nbr_agg, coarse_row):
    elems = a_blocks.shape[0]
    devices = elems // E_DEV
    owner_device = (jnp.arange(elems, dtype=jnp.int32) // E_DEV).astype(jnp.int32)
    agg_of = touch_agg[owner_device, elem_slot]
    valid = nbr >= 0
    safe_nbr = jnp.where(valid, nbr, 0).astype(jnp.int32)

    def per_device(index):
        start = (index * E_DEV).astype(jnp.int32)
        blocks = lax.dynamic_slice_in_dim(a_blocks, start, E_DEV, 0).astype(jnp.float32)
        left = lax.dynamic_slice_in_dim(prolong_t, start, E_DEV, 0)
        left_blocks = jnp.einsum("ecb,ekbd->ekcd", left.astype(jnp.float32), blocks,
                                 precision=lax.Precision.HIGHEST).astype(jnp.bfloat16)
        across = lax.dynamic_slice_in_dim(safe_nbr, start, E_DEV, 0)
        right = jnp.concatenate([left[:, None], prolong_t[across]], axis=1)
        products = jnp.einsum("ekcd,ekxd->ekcx", left_blocks.astype(jnp.float32), right.astype(jnp.float32),
                              precision=lax.Precision.HIGHEST)
        return products.reshape(E_DEV, 7, C * C)

    products = lax.map(per_device, jnp.arange(devices, dtype=jnp.int32)).reshape(elems, 7, C * C)
    same = valid & (nbr_agg == agg_of[:, None])
    apart = valid & jnp.logical_not(same)
    faces = products[:, 1:]
    diagonal = products[:, 0] + jnp.sum(jnp.where(same[:, :, None], faces, jnp.float32(0.0)), axis=1)
    contrib = jnp.concatenate([diagonal[:, None], jnp.where(apart[:, :, None], faces, jnp.float32(0.0))], axis=1)
    coarse_sum = jax.ops.segment_sum(contrib, agg_of, num_segments=AGG)
    coarse = jnp.zeros((COARSE, 7, C * C), jnp.float32).at[coarse_row].set(coarse_sum)
    return coarse
```

```python
import functools

import jax
import jax.numpy as jnp
from jax import lax
from jax.experimental import pallas as pl
from jax.experimental.pallas import tpu as pltpu
from jax.sharding import PartitionSpec as P

EX = 4
EY = 4
MESH = pl.DeviceIdType.MESH
F32 = jnp.float32
BF16 = jnp.bfloat16


def iota(shape, dim):
    return lax.broadcasted_iota(jnp.int32, shape, dim)


def tables(
    n_grp, n_dev, halo, group_rows, rows_own,
    nbr, nbr_agg, slot, touch_agg, coarse_row,
    tab, code,
):
    grp = lax.axis_index("grp")
    dev = lax.axis_index("dev")
    device = grp * n_dev + dev
    faces, e_dev = nbr.shape
    touch, devices = touch_agg.shape
    lane = code.shape[1]
    groups = code.shape[0] // (faces + 1)
    rep = e_dev // groups

    def where_sum(mask, value, axis):
        return jnp.sum(jnp.where(mask, value, 0), axis=axis, keepdims=True)

    def put(row, value):
        tab[row:row + value.shape[0], 0:value.shape[1]] = value

    near = [
        jnp.where(grp > 0, device - n_dev, -2),
        jnp.where(grp < n_grp - 1, device + n_dev, -2),
        jnp.where(dev > 0, device - 1, -2),
        jnp.where(dev < n_dev - 1, device + 1, -2),
    ]
    ids = nbr[...]
    source = jnp.where(ids >= 0, jnp.maximum(ids, 0) // e_dev, -1)
    local = ids - source * e_dev
    hits = [jnp.max(jnp.where(source == n, 1.0, 0.0), axis=0, keepdims=True) for n in near]
    below = jnp.where(iota((e_dev, e_dev), 0) < iota((e_dev, e_dev), 1), 1.0, 0.0).astype(BF16)
    rank = jnp.dot(
        jnp.concatenate(hits + hits, axis=0).astype(BF16), below, preferred_element_type=F32
    ).astype(jnp.int32)
    lanes = iota((halo, e_dev), 1)
    for d in range(4):
        found = (rank[d:d + 1] == iota((halo, e_dev), 0)) & (hits[d] > 0)
        tab[8:8 + halo, d:d + 1] = where_sum(found, lanes, 1)
    index = iota((e_dev, e_dev), 0)
    where_from = [jnp.where(source[f:f + 1] == device, local[f:f + 1], 0) for f in range(faces)]
    for d in range(4):
        seen = jnp.zeros((e_dev, e_dev), jnp.int32)
        for f in range(faces):
            seen = jnp.where(ids[f:f + 1] == near[d] * e_dev + index, 1, seen)
        seen = jnp.max(seen, axis=1, keepdims=True)
        for f in range(faces):
            ahead = where_sum(index < local[f:f + 1], seen, 0)
            where_from[f] = jnp.where(
                source[f:f + 1] == near[d], e_dev + d * halo + ahead, where_from[f]
            )
    for f in range(faces):
        put(f, where_from[f])

    row = iota((devices, 1), 0)
    entries = touch_agg[...].T
    columns = [entries[:, t:t + 1] for t in range(touch)]
    slots = slot[...]
    put(19, slots)
    own_agg = jnp.zeros((1, e_dev), jnp.int32)
    for t in range(touch):
        own_agg = jnp.where(slots == t, where_sum(row == device, columns[t], 0), own_agg)
    valid = ids >= 0
    same = valid & (nbr_agg[...] == own_agg)
    kind = jnp.where(same, slots + touch, jnp.where(valid, slots, -1))
    kind = jnp.concatenate([slots + touch, kind], axis=0).astype(F32)
    mine = iota((groups, e_dev), 1) // rep == iota((groups, e_dev), 0)
    tall = jnp.concatenate(
        [jnp.where(mine, kind[k:k + 1], 0.0) for k in range(faces + 1)], axis=0
    ).astype(BF16)
    place = iota((e_dev, lane), 0) % rep == iota((e_dev, lane), 1) // (lane // rep)
    place = jnp.where(place, 1.0, 0.0).astype(BF16)
    code[...] = jnp.dot(tall, place, preferred_element_type=F32).astype(jnp.int32)

    n_agg = coarse_row.shape[1]
    numbers = coarse_row[...]
    across = iota((devices, n_agg), 1)
    targets = [where_sum(columns[t] == across, numbers, 1) for t in range(touch)]
    owners = [target // rows_own for target in targets]
    lane = iota((devices, rows_own), 1)
    present = jnp.zeros((devices, rows_own), F32)
    for t in range(touch):
        here = jnp.where(owners[t] == dev, targets[t] - owners[t] * rows_own, -1)
        present = jnp.where(here == lane, 1.0, present)
    mates = jnp.where(
        iota((devices, devices), 0) // n_dev == iota((devices, devices), 1) // n_dev, 1.0, 0.0
    ).astype(BF16)
    shared = jnp.dot(mates, present.astype(BF16), preferred_element_type=F32) > 0
    shared = jnp.where(shared, 1.0, 0.0)
    lower = jnp.where(
        iota((rows_own, rows_own), 0) < iota((rows_own, rows_own), 1), 1.0, 0.0
    ).astype(BF16)
    order = jnp.dot(shared.astype(BF16), lower, preferred_element_type=F32)
    heads = where_sum(row % n_dev == 0, shared * (order + 1.0 + (row // n_dev * group_rows).astype(F32)), 0)
    put(16, heads.astype(jnp.int32) - 1)
    spots = jnp.sum(present * (order + 1.0), axis=1, keepdims=True).astype(jnp.int32) - 1
    peer = iota((devices, n_dev), 1) + grp * n_dev
    put(18, where_sum(peer == iota((devices, n_dev), 0), spots, 0))
    inverse = jnp.full((1, n_dev), touch, jnp.int32)
    for t in range(touch):
        own = where_sum(row == device, owners[t], 0)
        inverse = jnp.where(own == iota((1, n_dev), 1), t, inverse)
    put(17, inverse)


def order_of(n_k):
    return list(range(1, n_k)) + [0]


def chunks_of(n_k):
    return [(p, 1) for p in range(n_k)]


def finish(tab, gathered, out_ref, flat):
    n_k, rows_own, row_width = out_ref.shape
    group_rows, sub, lane = gathered.shape[2:]

    @pl.loop(0, rows_own, unroll=4)
    def _(r):
        at = tab[16, r]
        safe = jnp.maximum(at, 0)
        for p, k in enumerate(order_of(n_k)):
            row = gathered[p, safe // group_rows, safe % group_rows].astype(F32)
            flat[k, pl.ds(pl.multiple_of(r * sub, sub), sub), :] = jnp.where(at >= 0, row, 0.0)

    for k in range(n_k):
        for j in range(sub):
            out_ref[k, :, j * lane:(j + 1) * lane] = flat[k, pl.ds(j, rows_own, stride=sub), :]


def kernel(
    n_grp, n_dev, halo, group_rows,
    tab, a_ref, p_ref, code,
    gathered,
    a_buf, pool, pack, turned, left, prod, same_sum, part_t, parts, inbox,
    a_sem, h_send, h_recv, x_send, x_recv, g_send, g_recv,
):
    grp = lax.axis_index("grp")
    dev = lax.axis_index("dev")
    e_dev, width_c, width_b = p_ref.shape
    n_k = a_ref.shape[1]
    touch, _, lane = same_sum.shape
    rep = lane // width_c
    sub = width_c // rep
    groups = e_dev // rep
    order = order_of(n_k)
    chunks = chunks_of(n_k)

    def a_copy(p):
        return pltpu.make_async_copy(a_ref.at[:, order[p]], a_buf.at[p], a_sem.at[p])

    for p in range(n_k):
        a_copy(p).start()

    barrier = pltpu.get_barrier_semaphore()
    for off in range(1, n_dev):
        pl.semaphore_signal(
            barrier, inc=1, device_id=(grp, lax.rem(dev + off, n_dev)), device_id_type=MESH
        )
    for off in range(1, n_grp):
        pl.semaphore_signal(
            barrier, inc=1, device_id=(lax.rem(grp + off, n_grp), dev), device_id_type=MESH
        )

    for j in range(4 * halo):
        pack[j] = p_ref[tab[8 + j % halo, j // halo]]
    pool[0:e_dev] = p_ref[...]
    turn = iota((width_c, width_c), 1) == iota((width_c, width_c), 0) % sub * rep + iota((width_c, width_c), 0) // sub
    turn = turn.astype(F32).astype(BF16)

    @pl.loop(0, e_dev, unroll=e_dev)
    def _(e):
        turned[e] = jnp.dot(turn, p_ref[e], preferred_element_type=F32).astype(BF16)

    same_sum[...] = jnp.zeros(same_sum.shape, F32)
    part_t[touch] = jnp.zeros(part_t.shape[1:], BF16)

    dirs = (
        (grp > 0, (grp - 1, dev)),
        (grp < n_grp - 1, (grp + 1, dev)),
        (dev > 0, (grp, dev - 1)),
        (dev < n_dev - 1, (grp, dev + 1)),
    )

    def halo_copy(d, target):
        back = d ^ 1
        return pltpu.make_async_remote_copy(
            src_ref=pack.at[pl.ds(d * halo, halo)],
            dst_ref=pool.at[pl.ds(e_dev + back * halo, halo)],
            send_sem=h_send.at[d],
            recv_sem=h_recv.at[back],
            device_id=target,
            device_id_type=MESH,
        )

    def halo_start():
        pl.semaphore_wait(barrier, n_dev + n_grp - 2)
        for d, (there, target) in enumerate(dirs):
            @pl.when(there)
            def _(d=d, target=target):
                halo_copy(d, target).start()

    def halo_wait():
        for d, (there, target) in enumerate(dirs):
            @pl.when(there)
            def _(d=d, target=target):
                halo_copy(d, target).wait_send()
                pltpu.make_async_remote_copy(
                    src_ref=pack.at[pl.ds(d * halo, halo)],
                    dst_ref=pool.at[pl.ds(e_dev + d * halo, halo)],
                    send_sem=h_send.at[d],
                    recv_sem=h_recv.at[d],
                    device_id=target,
                    device_id_type=MESH,
                ).wait_recv()

    def left_of(p):
        a_copy(p).wait()

        @pl.loop(0, e_dev, unroll=e_dev)
        def _(e):
            rows = pl.ds(pl.multiple_of(e * width_c, width_c), width_c)
            left[p, rows, :] = jnp.dot(
                turned[e], a_buf[p, e], preferred_element_type=F32
            ).astype(BF16)

    group_of_lane = iota((width_c, lane), 1) // width_c
    sub_lane = iota((sub, lane), 1) // width_c

    def squeeze(total):
        pieces = [total[j * sub:(j + 1) * sub] for j in range(rep)]
        out = None
        for s in range(rep):
            picked = pieces[s]
            for g in range(1, rep):
                picked = jnp.where(sub_lane == g, pieces[(g + s) % rep], picked)
            if s:
                picked = pltpu.roll(picked, s * width_c, 1)
            out = picked if out is None else out + picked
        return out

    def right_of(p):
        k = order[p]

        @pl.loop(0, groups, unroll=groups)
        def _(g):
            if k:
                blocks = [pool[tab[k - 1, g * rep + i]] for i in range(rep)]
            else:
                blocks = [p_ref[g * rep + i] for i in range(rep)]
            rows = pl.ds(pl.multiple_of(g * lane, lane), lane)
            full = lax.dot_general(
                left[p, rows, :], jnp.concatenate(blocks, axis=0),
                (((1,), (1,)), ((), ())), preferred_element_type=F32,
            )
            picked = full[0:width_c]
            for i in range(1, rep):
                picked = jnp.where(group_of_lane == i, full[i * width_c:(i + 1) * width_c], picked)
            prod[g] = picked

        def masked(t):
            total = None
            for g in range(groups):
                at = k * groups + g
                term = jnp.where(code[at:at + 1, :] == t, prod[g], 0.0)
                total = term if total is None else total + term
            return total

        for t in range(touch):
            same_sum[t] += masked(t + touch)
            part_t[t] = squeeze(masked(t) if k else same_sum[t]).astype(BF16)
        for o in range(n_dev):
            parts[p, o] = part_t[tab[17, o]]
        inbox[p, dev] = parts[p, dev]

    def part_copy(c, off):
        start, size = chunks[c]
        target = lax.rem(dev + off, n_dev)
        return pltpu.make_async_remote_copy(
            src_ref=parts.at[pl.ds(start, size), target],
            dst_ref=inbox.at[pl.ds(start, size), dev],
            send_sem=x_send.at[c, off],
            recv_sem=x_recv.at[c, off],
            device_id=(grp, target),
            device_id_type=MESH,
        )

    def part_arrival(c, off):
        start, size = chunks[c]
        sender = lax.rem(dev + n_dev - off, n_dev)
        return pltpu.make_async_remote_copy(
            src_ref=parts.at[pl.ds(start, size), sender],
            dst_ref=inbox.at[pl.ds(start, size), sender],
            send_sem=x_send.at[c, off],
            recv_sem=x_recv.at[c, off],
            device_id=(grp, sender),
            device_id_type=MESH,
        )

    def row_copy(c, off):
        start, size = chunks[c]
        target = lax.rem(grp + off, n_grp)
        return pltpu.make_async_remote_copy(
            src_ref=gathered.at[pl.ds(start, size), grp],
            dst_ref=gathered.at[pl.ds(start, size), grp],
            send_sem=g_send.at[c, off],
            recv_sem=g_recv.at[c, off],
            device_id=(target, dev),
            device_id_type=MESH,
        )

    def row_arrival(c, off):
        start, size = chunks[c]
        sender = lax.rem(grp + n_grp - off, n_grp)
        return pltpu.make_async_remote_copy(
            src_ref=gathered.at[pl.ds(start, size), sender],
            dst_ref=gathered.at[pl.ds(start, size), sender],
            send_sem=g_send.at[c, off],
            recv_sem=g_recv.at[c, off],
            device_id=(sender, dev),
            device_id_type=MESH,
        )

    def exchange(c):
        for off in range(1, n_dev):
            part_copy(c, off).start()

    def collect(c):
        for off in range(1, n_dev):
            part_arrival(c, off).wait_recv()
        start, size = chunks[c]
        for p in range(start, start + size):
            for j in range(group_rows):
                total = jnp.zeros((sub, lane), F32)
                for d in range(n_dev):
                    member = jnp.where(tab[18, d] == j, 1.0, 0.0).astype(F32)
                    total = total + inbox[p, d].astype(F32) * member
                gathered[p, grp, j] = total.astype(BF16)
        for off in range(1, n_grp):
            row_copy(c, off).start()

    left_of(0)
    halo_start()
    left_of(1)
    left_of(2)
    left_of(3)
    left_of(4)
    left_of(5)
    halo_wait()
    right_of(0)
    exchange(0)
    right_of(1)
    exchange(1)
    right_of(2)
    exchange(2)
    right_of(3)
    exchange(3)
    right_of(4)
    exchange(4)
    collect(0)
    right_of(5)
    exchange(5)
    collect(1)
    left_of(6)
    collect(2)
    right_of(6)
    exchange(6)
    collect(3)
    collect(4)
    collect(5)
    collect(6)

    for c in range(len(chunks)):
        for off in range(1, n_dev):
            part_copy(c, off).wait_send()
    for c in range(len(chunks)):
        for off in range(1, n_grp):
            row_arrival(c, off).wait_recv()
            row_copy(c, off).wait_send()


def on_device(n_grp, n_dev, a_blocks, prolong_t, elem_slot, touch_agg, nbr, nbr_agg, coarse_row):
    e_dev, width_c, width_b = prolong_t.shape
    n_k = a_blocks.shape[1]
    touch = touch_agg.shape[1]
    halo = e_dev // EX
    half_y = EY // 2
    span_y = half_y + 1
    group_rows = (n_dev * half_y + 1 + half_y) // span_y
    rows_own = n_grp * group_rows
    assert touch <= n_dev
    lane = 128
    rep = lane // width_c
    sub = width_c // rep
    groups = e_dev // rep
    n_chunks = len(chunks_of(n_k))
    smem = pl.BlockSpec(memory_space=pltpu.SMEM)
    vmem = pl.BlockSpec(memory_space=pltpu.VMEM)
    tab, code = pl.pallas_call(
        functools.partial(tables, n_grp, n_dev, halo, group_rows, rows_own),
        out_shape=(
            jax.ShapeDtypeStruct((24, lane), jnp.int32),
            jax.ShapeDtypeStruct((n_k * groups, lane), jnp.int32),
        ),
        in_specs=[vmem] * 5,
        out_specs=(vmem, vmem),
        name="index_tables",
    )(nbr.T, nbr_agg.T, elem_slot.reshape(1, e_dev), touch_agg.T, coarse_row.reshape(1, -1))
    gathered = pl.pallas_call(
        functools.partial(kernel, n_grp, n_dev, halo, group_rows),
        out_shape=jax.ShapeDtypeStruct((n_k, n_grp, group_rows, sub, lane), BF16),
        in_specs=[smem, pl.BlockSpec(memory_space=pl.ANY)] + [vmem] * 2,
        out_specs=vmem,
        scratch_shapes=[
            pltpu.VMEM((n_k, e_dev, width_b, width_b), BF16),
            pltpu.VMEM((e_dev + 4 * halo, width_c, width_b), BF16),
            pltpu.VMEM((4 * halo, width_c, width_b), BF16),
            pltpu.VMEM((e_dev, width_c, width_b), BF16),
            pltpu.VMEM((n_k, e_dev * width_c, width_b), BF16),
            pltpu.VMEM((groups, width_c, lane), F32),
            pltpu.VMEM((touch, width_c, lane), F32),
            pltpu.VMEM((touch + 1, sub, lane), BF16),
            pltpu.VMEM((n_k, n_dev, sub, lane), BF16),
            pltpu.VMEM((n_k, n_dev, sub, lane), BF16),
            pltpu.SemaphoreType.DMA((n_k,)),
            pltpu.SemaphoreType.DMA((4,)),
            pltpu.SemaphoreType.DMA((4,)),
            pltpu.SemaphoreType.DMA((n_chunks, n_dev)),
            pltpu.SemaphoreType.DMA((n_chunks, n_dev)),
            pltpu.SemaphoreType.DMA((n_chunks, n_grp)),
            pltpu.SemaphoreType.DMA((n_chunks, n_grp)),
        ],
        compiler_params=pltpu.CompilerParams(
            collective_id=0, has_side_effects=True, vmem_limit_bytes=60 * 1024 * 1024
        ),
        name="galerkin",
    )(tab, a_blocks, prolong_t, code)
    out = pl.pallas_call(
        finish,
        out_shape=jax.ShapeDtypeStruct((n_k, rows_own, width_c * width_c), F32),
        in_specs=[smem, vmem],
        out_specs=vmem,
        scratch_shapes=[pltpu.VMEM((n_k, rows_own * sub, lane), F32)],
        name="index_finish",
    )(tab, gathered)
    return out.transpose(1, 0, 2)


def solution(mesh):
    in_specs = (
        P(("grp", "dev"), None, None, None),
        P(("grp", "dev"), None, None),
        P(("grp", "dev")),
        P(),
        P(("grp", "dev"), None),
        P(("grp", "dev"), None),
        P(),
    )
    out_specs = P("dev", None, None)
    return jax.shard_map(
        functools.partial(on_device, mesh.shape["grp"], mesh.shape["dev"]),
        mesh=mesh, in_specs=in_specs, out_specs=out_specs, check_vma=False,
    )
```

```python
import functools

import jax
import jax.numpy as jnp
from jax import lax
from jax.experimental import pallas as pl
from jax.experimental.pallas import tpu as pltpu
from jax.sharding import PartitionSpec as P

EX = 4
EY = 4
MESH = pl.DeviceIdType.MESH
F32 = jnp.float32
BF16 = jnp.bfloat16


def iota(shape, dim):
    return lax.broadcasted_iota(jnp.int32, shape, dim)


def where_sum(mask, value, axis):
    return jnp.sum(jnp.where(mask, value, 0), axis=axis, keepdims=True)


def ones(mask):
    return jnp.where(mask, 1.0, 0.0).astype(BF16)


def place_of(k, n_k):
    return (k + n_k - 1) % n_k


def chunks_of(n_k):
    return [(p, 1) for p in range(n_k - 2)] + [(n_k - 2, 2)]


def halo_tables(grp, dev, n_grp, n_dev, halo, nbr, tab):
    device = grp * n_dev + dev
    faces, e_dev = nbr.shape
    near = [
        jnp.where(grp > 0, device - n_dev, -2),
        jnp.where(grp < n_grp - 1, device + n_dev, -2),
        jnp.where(dev > 0, device - 1, -2),
        jnp.where(dev < n_dev - 1, device + 1, -2),
    ]
    ids = nbr
    source = jnp.where(ids >= 0, jnp.maximum(ids, 0) // e_dev, -1)
    local = ids - source * e_dev
    hits = [jnp.max(jnp.where(source == n, 1.0, 0.0), axis=0, keepdims=True) for n in near]
    below = ones(iota((e_dev, e_dev), 0) < iota((e_dev, e_dev), 1))
    rank = jnp.dot(
        jnp.concatenate(hits + hits, axis=0).astype(BF16), below, preferred_element_type=F32
    ).astype(jnp.int32)
    lanes = iota((halo, e_dev), 1)
    tab[...] = jnp.zeros(tab.shape, jnp.int32)
    for d in range(4):
        found = (rank[d:d + 1] == iota((halo, e_dev), 0)) & (hits[d] > 0)
        tab[8:8 + halo, d:d + 1] = where_sum(found, lanes, 1)
    index = iota((e_dev, e_dev), 0)
    where_from = [jnp.where(source[f:f + 1] == device, local[f:f + 1], 0) for f in range(faces)]
    for d in range(4):
        seen = jnp.zeros((e_dev, e_dev), jnp.int32)
        for f in range(faces):
            seen = jnp.where(ids[f:f + 1] == near[d] * e_dev + index, 1, seen)
        seen = jnp.max(seen, axis=1, keepdims=True)
        for f in range(faces):
            ahead = where_sum(index < local[f:f + 1], seen, 0)
            where_from[f] = jnp.where(
                source[f:f + 1] == near[d], e_dev + d * halo + ahead, where_from[f]
            )
    for f in range(faces):
        tab[f:f + 1, 0:e_dev] = where_from[f]


def owner_tables(
    grp, dev, n_dev, group_rows, rows_own,
    nbr, nbr_agg, slot, touch_agg, coarse_row, tab, code,
):
    device = grp * n_dev + dev
    faces, e_dev = nbr.shape
    touch, devices = touch_agg.shape
    lane = code.shape[1]
    groups = code.shape[0] // (faces + 1)
    rep = e_dev // groups

    def put(row, value):
        tab[row:row + 1, 0:value.shape[1]] = value

    ids = nbr
    row = iota((devices, 1), 0)
    entries = touch_agg.T
    columns = [entries[:, t:t + 1] for t in range(touch)]
    slots = slot
    own_agg = jnp.zeros((1, e_dev), jnp.int32)
    for t in range(touch):
        own_agg = jnp.where(slots == t, where_sum(row == device, columns[t], 0), own_agg)
    valid = ids >= 0
    same = valid & (nbr_agg == own_agg)
    kind = jnp.where(same, slots + touch, jnp.where(valid, slots, -1))
    kind = jnp.concatenate([slots + touch, kind], axis=0).astype(F32)
    mine = iota((groups, e_dev), 1) // rep == iota((groups, e_dev), 0)
    tall = jnp.concatenate(
        [jnp.where(mine, kind[k:k + 1], 0.0) for k in range(faces + 1)], axis=0
    ).astype(BF16)
    place = ones(iota((e_dev, lane), 0) % rep == iota((e_dev, lane), 1) // (lane // rep))
    code[...] = jnp.dot(tall, place, preferred_element_type=F32).astype(jnp.int32)

    n_agg = coarse_row.shape[1]
    numbers = coarse_row
    across = iota((devices, n_agg), 1)
    targets = [where_sum(columns[t] == across, numbers, 1) for t in range(touch)]
    owners = [target // rows_own for target in targets]
    spot = iota((devices, rows_own), 1)
    present = jnp.zeros((devices, rows_own), F32)
    for t in range(touch):
        here = jnp.where(owners[t] == dev, targets[t] - owners[t] * rows_own, -1)
        present = jnp.where(here == spot, 1.0, present)
    mates = ones(iota((devices, devices), 0) // n_dev == iota((devices, devices), 1) // n_dev)
    shared = jnp.dot(mates, present.astype(BF16), preferred_element_type=F32) > 0
    shared = jnp.where(shared, 1.0, 0.0)
    lower = ones(iota((rows_own, rows_own), 0) < iota((rows_own, rows_own), 1))
    order = jnp.dot(shared.astype(BF16), lower, preferred_element_type=F32)
    heads = where_sum(row % n_dev == 0, shared * (order + 1.0 + (row // n_dev * group_rows).astype(F32)), 0)
    tab[...] = jnp.zeros(tab.shape, jnp.int32)
    put(0, jnp.minimum(heads.astype(jnp.int32), rows_own) - 1)
    spots = jnp.sum(present * (order + 1.0), axis=1, keepdims=True).astype(jnp.int32) - 1
    peer = iota((devices, n_dev), 1) + grp * n_dev
    put(2, where_sum(peer == iota((devices, n_dev), 0), spots, 0))
    inverse = jnp.full((1, n_dev), touch, jnp.int32)
    for t in range(touch):
        own = where_sum(row == device, owners[t], 0)
        inverse = jnp.where(own == iota((1, n_dev), 1), t, inverse)
    put(1, inverse)


def kernel(
    n_grp, n_dev, halo, group_rows, rows_own, n_agg,
    a_ref, p_ref, packed,
    out_ref,
    near_v, own_v, near, own, code,
    a_buf, p_buf, pool, pack, turned, left, prod, same_sum, part_t, parts, inbox, flat,
    *rest,
):
    *gathered, a_sem, p_sem, t_sem, h_send, h_recv, x_send, x_recv, g_send, g_recv = rest
    grp = lax.axis_index("grp")
    dev = lax.axis_index("dev")
    e_dev, width_c, width_b = p_ref.shape
    n_k = a_ref.shape[1]
    touch, _, lane = same_sum.shape
    rep = lane // width_c
    sub = width_c // rep
    groups = e_dev // rep
    chunks = chunks_of(n_k)
    parted = a_sem.shape[1]

    def a_copies(k):
        count = parted if k == 0 else 1
        size = e_dev // count
        return [
            pltpu.make_async_copy(
                a_ref.at[pl.ds(q * size, size), k], a_buf.at[k, pl.ds(q * size, size)], a_sem.at[k, q]
            )
            for q in range(count)
        ]

    faces = n_k - 1
    nbr = packed[0:faces, 0:e_dev]
    nbr_agg = packed[8:8 + faces, 0:e_dev]
    touch_agg = packed[16:16 + touch, 0:n_grp * n_dev]
    slot = packed[24:25, 0:e_dev]
    coarse_row = packed[32:33, 0:n_agg]
    p_copy = pltpu.make_async_copy(p_ref, p_buf, p_sem.at[0])
    near_copy = pltpu.make_async_copy(near_v, near, t_sem.at[0])
    own_copy = pltpu.make_async_copy(own_v, own, t_sem.at[1])
    p_copy.start()

    barrier = pltpu.get_barrier_semaphore()
    for off in range(1, n_dev):
        pl.semaphore_signal(
            barrier, inc=1, device_id=(grp, lax.rem(dev + off, n_dev)), device_id_type=MESH
        )
    for off in range(1, n_grp):
        pl.semaphore_signal(
            barrier, inc=1, device_id=(lax.rem(grp + off, n_grp), dev), device_id_type=MESH
        )

    dirs = (
        (grp > 0, (grp - 1, dev)),
        (grp < n_grp - 1, (grp + 1, dev)),
        (dev > 0, (grp, dev - 1)),
        (dev < n_dev - 1, (grp, dev + 1)),
    )

    def halo_copy(d, target):
        back = d ^ 1
        return pltpu.make_async_remote_copy(
            src_ref=pack.at[pl.ds(d * halo, halo)],
            dst_ref=pool.at[pl.ds(e_dev + back * halo, halo)],
            send_sem=h_send.at[d],
            recv_sem=h_recv.at[back],
            device_id=target,
            device_id_type=MESH,
        )

    def tables_one():
        halo_tables(grp, dev, n_grp, n_dev, halo, nbr, near_v)
        near_copy.start()

    def tables_two():
        owner_tables(
            grp, dev, n_dev, group_rows, rows_own,
            nbr, nbr_agg, slot, touch_agg, coarse_row, own_v, code,
        )
        part_t[touch] = jnp.zeros(part_t.shape[1:], BF16)
        own_copy.start()

    def a_first():
        for copy in a_copies(0):
            copy.start()

    def p_wait():
        p_copy.wait()
        for k in range(1, n_k):
            for copy in a_copies(k):
                copy.start()

    def turn_p():
        turn = ones(
            iota((width_c, width_c), 1)
            == iota((width_c, width_c), 0) % sub * rep + iota((width_c, width_c), 0) // sub
        )

        @pl.loop(0, e_dev, unroll=e_dev)
        def _(e):
            turned[e] = jnp.dot(turn, p_buf[e], preferred_element_type=F32).astype(BF16)

    def halo_start():
        near_copy.wait()
        for j in range(4 * halo):
            pack[j] = p_buf[near[8 + j % halo, j // halo]]
        pool[0:e_dev] = p_buf[...]
        pl.semaphore_wait(barrier, n_dev + n_grp - 2)
        for d, (there, target) in enumerate(dirs):
            @pl.when(there)
            def _(d=d, target=target):
                halo_copy(d, target).start()

    def halo_wait():
        for d, (there, target) in enumerate(dirs):
            @pl.when(there)
            def _(d=d, target=target):
                halo_copy(d, target).wait_send()
                pltpu.make_async_remote_copy(
                    src_ref=pack.at[pl.ds(d * halo, halo)],
                    dst_ref=pool.at[pl.ds(e_dev + d * halo, halo)],
                    send_sem=h_send.at[d],
                    recv_sem=h_recv.at[d],
                    device_id=target,
                    device_id_type=MESH,
                ).wait_recv()

    def left_of(k):
        copies = a_copies(k)
        for q, copy in enumerate(copies):
            copy.wait()
            size = e_dev // len(copies)

            @pl.loop(q * size, (q + 1) * size, unroll=size)
            def _(e):
                rows = pl.ds(pl.multiple_of(e * width_c, width_c), width_c)
                left[k, rows, :] = jnp.dot(
                    turned[e], a_buf[k, e], preferred_element_type=F32
                ).astype(BF16)

    group_of_lane = iota((width_c, lane), 1) // width_c
    sub_lane = iota((sub, lane), 1) // width_c

    def squeeze(total):
        pieces = [total[j * sub:(j + 1) * sub] for j in range(rep)]
        out = None
        for s in range(rep):
            picked = pieces[s]
            for g in range(1, rep):
                picked = jnp.where(sub_lane == g, pieces[(g + s) % rep], picked)
            if s:
                picked = pltpu.roll(picked, s * width_c, 1)
            out = picked if out is None else out + picked
        return out

    def right_of(k):
        @pl.loop(0, groups, unroll=groups)
        def _(g):
            if k:
                blocks = [pool[near[k - 1, g * rep + i]] for i in range(rep)]
            else:
                blocks = [p_buf[g * rep + i] for i in range(rep)]
            rows = pl.ds(pl.multiple_of(g * lane, lane), lane)
            full = lax.dot_general(
                left[k, rows, :], jnp.concatenate(blocks, axis=0),
                (((1,), (1,)), ((), ())), preferred_element_type=F32,
            )
            picked = full[0:width_c]
            for i in range(1, rep):
                picked = jnp.where(group_of_lane == i, full[i * width_c:(i + 1) * width_c], picked)
            prod[k % 2, g] = picked

        def masked(t):
            total = None
            for g in range(groups):
                at = k * groups + g
                term = jnp.where(code[at:at + 1, :] == t, prod[k % 2, g], 0.0)
                total = term if total is None else total + term
            return total

        for t in range(touch):
            together = masked(t + touch)
            if k:
                together = same_sum[t] + together
            same_sum[t] = together
            if k:
                part_t[t] = squeeze(masked(t)).astype(BF16)
        if k:
            emit(k)
        if k == n_k - 1:
            for t in range(touch):
                part_t[t] = squeeze(same_sum[t]).astype(BF16)
            emit(0)

    def emit(k):
        p = place_of(k, n_k)
        for o in range(n_dev):
            parts[p, o] = part_t[own[1, o]]
        inbox[p, dev] = parts[p, dev]

    def part_copy(c, off):
        start, size = chunks[c]
        target = lax.rem(dev + off, n_dev)
        return pltpu.make_async_remote_copy(
            src_ref=parts.at[pl.ds(start, size), target],
            dst_ref=inbox.at[pl.ds(start, size), dev],
            send_sem=x_send.at[c, off],
            recv_sem=x_recv.at[c, off],
            device_id=(grp, target),
            device_id_type=MESH,
        )

    def part_arrival(c, off):
        start, size = chunks[c]
        sender = lax.rem(dev + n_dev - off, n_dev)
        return pltpu.make_async_remote_copy(
            src_ref=parts.at[pl.ds(start, size), sender],
            dst_ref=inbox.at[pl.ds(start, size), sender],
            send_sem=x_send.at[c, off],
            recv_sem=x_recv.at[c, off],
            device_id=(grp, sender),
            device_id_type=MESH,
        )

    def row_copy(c, off):
        target = lax.rem(grp + off, n_grp)
        return pltpu.make_async_remote_copy(
            src_ref=gathered[c].at[pl.ds(grp * group_rows, group_rows)],
            dst_ref=gathered[c].at[pl.ds(grp * group_rows, group_rows)],
            send_sem=g_send.at[c, off],
            recv_sem=g_recv.at[c, off],
            device_id=(target, dev),
            device_id_type=MESH,
        )

    def row_arrival(c, off):
        sender = lax.rem(grp + n_grp - off, n_grp)
        return pltpu.make_async_remote_copy(
            src_ref=gathered[c].at[pl.ds(sender * group_rows, group_rows)],
            dst_ref=gathered[c].at[pl.ds(sender * group_rows, group_rows)],
            send_sem=g_send.at[c, off],
            recv_sem=g_recv.at[c, off],
            device_id=(sender, dev),
            device_id_type=MESH,
        )

    def exchange(c):
        for off in range(1, n_dev):
            part_copy(c, off).start()

    def collect(c):
        for off in range(1, n_dev):
            part_arrival(c, off).wait_recv()
        start, size = chunks[c]
        for j in range(group_rows):
            for i in range(size):
                total = jnp.zeros((sub, lane), F32)
                for d in range(n_dev):
                    member = jnp.where(own[2, d] == j, 1.0, 0.0).astype(F32)
                    total = total + inbox[start + i, d].astype(F32) * member
                gathered[c][grp * group_rows + j, i] = total.astype(BF16)
        for off in range(1, n_grp):
            row_copy(c, off).start()

    def place(c):
        for off in range(1, n_grp):
            row_arrival(c, off).wait_recv()
        start, size = chunks[c]
        for i in range(size):
            k = (start + i + 1) % n_k

            @pl.loop(0, rows_own, unroll=8)
            def _(r, i=i):
                at = own[0, r]
                row = gathered[c][jnp.maximum(at, 0), i].astype(F32)
                flat[i, pl.ds(pl.multiple_of(r * sub, sub), sub), :] = jnp.where(at >= 0, row, 0.0)

            for j in range(sub):
                out_ref[k, :, j * lane:(j + 1) * lane] = flat[i, pl.ds(j, rows_own, stride=sub), :].astype(BF16)

    def sent():
        for c in range(len(chunks)):
            for off in range(1, n_dev):
                part_copy(c, off).wait_send()
            for off in range(1, n_grp):
                row_copy(c, off).wait_send()

    tables_one()
    a_first()
    tables_two()
    p_wait()
    halo_start()
    turn_p()
    left_of(0)
    own_copy.wait()
    right_of(0)
    left_of(1)
    left_of(2)
    halo_wait()
    right_of(1)
    exchange(0)
    left_of(3)
    right_of(2)
    exchange(1)
    left_of(4)
    right_of(3)
    exchange(2)
    left_of(5)
    right_of(4)
    exchange(3)
    collect(0)
    left_of(6)
    right_of(5)
    exchange(4)
    collect(1)
    right_of(6)
    exchange(5)
    collect(2)
    collect(3)
    collect(4)
    place(0)
    place(1)
    collect(5)
    place(2)
    place(3)
    place(4)
    place(5)
    sent()


def on_device(n_grp, n_dev, a_blocks, prolong_t, elem_slot, touch_agg, nbr, nbr_agg, coarse_row):
    e_dev, width_c, width_b = prolong_t.shape
    n_k = a_blocks.shape[1]
    touch = touch_agg.shape[1]
    halo = e_dev // EX
    half_y = EY // 2
    span_y = half_y + 1
    group_rows = (n_dev * half_y + 1 + half_y) // span_y
    rows_own = n_grp * group_rows
    assert touch <= n_dev
    lane = 128
    rep = lane // width_c
    sub = width_c // rep
    groups = e_dev // rep
    chunks = chunks_of(n_k)
    n_chunks = len(chunks)
    parted = 2
    hbm = pl.BlockSpec(memory_space=pltpu.HBM)
    vmem = pl.BlockSpec(memory_space=pltpu.VMEM)
    ints = [nbr.T, nbr_agg.T, touch_agg.T, elem_slot.reshape(1, e_dev), coarse_row.reshape(1, -1)]
    width = -(-max(x.shape[1] for x in ints) // lane) * lane
    packed = sum(
        jnp.pad(x, ((8 * i, 8 * (len(ints) - i) - x.shape[0]), (0, width - x.shape[1])))
        for i, x in enumerate(ints)
    )
    out = pl.pallas_call(
        functools.partial(kernel, n_grp, n_dev, halo, group_rows, rows_own, coarse_row.shape[0]),
        out_shape=jax.ShapeDtypeStruct((n_k, rows_own, width_c * width_c), BF16),
        in_specs=[hbm] * 2 + [vmem],
        out_specs=vmem,
        scratch_shapes=[
            pltpu.VMEM((16, lane), jnp.int32),
            pltpu.VMEM((8, lane), jnp.int32),
            pltpu.SMEM((16, lane), jnp.int32),
            pltpu.SMEM((8, lane), jnp.int32),
            pltpu.VMEM((n_k * groups, lane), jnp.int32),
            pltpu.VMEM((n_k, e_dev, width_b, width_b), BF16),
            pltpu.VMEM((e_dev, width_c, width_b), BF16),
            pltpu.VMEM((e_dev + 4 * halo, width_c, width_b), BF16),
            pltpu.VMEM((4 * halo, width_c, width_b), BF16),
            pltpu.VMEM((e_dev, width_c, width_b), BF16),
            pltpu.VMEM((n_k, e_dev * width_c, width_b), BF16),
            pltpu.VMEM((2, groups, width_c, lane), F32),
            pltpu.VMEM((touch, width_c, lane), F32),
            pltpu.VMEM((touch + 1, sub, lane), BF16),
            pltpu.VMEM((n_k, n_dev, sub, lane), BF16),
            pltpu.VMEM((n_k, n_dev, sub, lane), BF16),
            pltpu.VMEM((2, rows_own * sub, lane), F32),
        ] + [pltpu.VMEM((rows_own, size, sub, lane), BF16) for _, size in chunks] + [
            pltpu.SemaphoreType.DMA((n_k, parted)),
            pltpu.SemaphoreType.DMA((1,)),
            pltpu.SemaphoreType.DMA((2,)),
            pltpu.SemaphoreType.DMA((4,)),
            pltpu.SemaphoreType.DMA((4,)),
            pltpu.SemaphoreType.DMA((n_chunks, n_dev)),
            pltpu.SemaphoreType.DMA((n_chunks, n_dev)),
            pltpu.SemaphoreType.DMA((n_chunks, n_grp)),
            pltpu.SemaphoreType.DMA((n_chunks, n_grp)),
        ],
        compiler_params=pltpu.CompilerParams(
            collective_id=0, has_side_effects=True, vmem_limit_bytes=54656 * 1024
        ),
        name="galerkin",
    )(a_blocks, prolong_t, packed)
    return out.astype(F32).transpose(1, 0, 2)


def solution(mesh):
    in_specs = (
        P(("grp", "dev"), None, None, None),
        P(("grp", "dev"), None, None),
        P(("grp", "dev")),
        P(),
        P(("grp", "dev"), None),
        P(("grp", "dev"), None),
        P(),
    )
    out_specs = P("dev", None, None)
    return jax.shard_map(
        functools.partial(on_device, mesh.shape["grp"], mesh.shape["dev"]),
        mesh=mesh, in_specs=in_specs, out_specs=out_specs, check_vma=False,
    )
```

```python
import functools

import jax
import jax.numpy as jnp
from jax import lax
from jax.experimental import pallas as pl
from jax.experimental.pallas import tpu as pltpu
from jax.sharding import PartitionSpec as P

EX = 4
EY = 4
MESH = pl.DeviceIdType.MESH
F32 = jnp.float32
BF16 = jnp.bfloat16


def iota(shape, dim):
    return lax.broadcasted_iota(jnp.int32, shape, dim)


def where_sum(mask, value, axis):
    return jnp.sum(jnp.where(mask, value, 0), axis=axis, keepdims=True)


def ones(mask):
    return jnp.where(mask, 1.0, 0.0).astype(BF16)


def place_of(k, n_k):
    return (k + n_k - 1) % n_k


def chunks_of(n_k):
    return [(p, 1) for p in range(n_k)]


def halo_tables(grp, dev, n_grp, n_dev, halo, nbr, tab):
    device = grp * n_dev + dev
    faces, e_dev = nbr.shape
    near = [
        jnp.where(grp > 0, device - n_dev, -2),
        jnp.where(grp < n_grp - 1, device + n_dev, -2),
        jnp.where(dev > 0, device - 1, -2),
        jnp.where(dev < n_dev - 1, device + 1, -2),
    ]
    ids = nbr
    source = jnp.where(ids >= 0, jnp.maximum(ids, 0) // e_dev, -1)
    local = ids - source * e_dev
    hits = [jnp.max(jnp.where(source == n, 1.0, 0.0), axis=0, keepdims=True) for n in near]
    below = ones(iota((e_dev, e_dev), 0) < iota((e_dev, e_dev), 1))
    rank = jnp.dot(
        jnp.concatenate(hits + hits, axis=0).astype(BF16), below, preferred_element_type=F32
    ).astype(jnp.int32)
    lanes = iota((halo, e_dev), 1)
    tab[...] = jnp.zeros(tab.shape, jnp.int32)
    for d in range(4):
        found = (rank[d:d + 1] == iota((halo, e_dev), 0)) & (hits[d] > 0)
        tab[8:8 + halo, d:d + 1] = where_sum(found, lanes, 1)
    index = iota((e_dev, e_dev), 0)
    where_from = [jnp.where(source[f:f + 1] == device, local[f:f + 1], 0) for f in range(faces)]
    for d in range(4):
        seen = jnp.zeros((e_dev, e_dev), jnp.int32)
        for f in range(faces):
            seen = jnp.where(ids[f:f + 1] == near[d] * e_dev + index, 1, seen)
        seen = jnp.max(seen, axis=1, keepdims=True)
        for f in range(faces):
            ahead = where_sum(index < local[f:f + 1], seen, 0)
            where_from[f] = jnp.where(
                source[f:f + 1] == near[d], e_dev + d * halo + ahead, where_from[f]
            )
    for f in range(faces):
        tab[f:f + 1, 0:e_dev] = where_from[f]


def owner_tables(
    grp, dev, n_dev, group_rows, rows_own,
    nbr, nbr_agg, slot, touch_agg, coarse_row, tab, code,
):
    device = grp * n_dev + dev
    faces, e_dev = nbr.shape
    touch, devices = touch_agg.shape
    lane = code.shape[1]
    groups = code.shape[0] // (faces + 1)
    rep = e_dev // groups

    def put(row, value):
        tab[row:row + 1, 0:value.shape[1]] = value

    ids = nbr
    row = iota((devices, 1), 0)
    entries = touch_agg.T
    columns = [entries[:, t:t + 1] for t in range(touch)]
    slots = slot
    own_agg = jnp.zeros((1, e_dev), jnp.int32)
    for t in range(touch):
        own_agg = jnp.where(slots == t, where_sum(row == device, columns[t], 0), own_agg)
    valid = ids >= 0
    same = valid & (nbr_agg == own_agg)
    kind = jnp.where(same, slots + touch, jnp.where(valid, slots, -1))
    kind = jnp.concatenate([slots + touch, kind], axis=0).astype(F32)
    mine = iota((groups, e_dev), 1) // rep == iota((groups, e_dev), 0)
    tall = jnp.concatenate(
        [jnp.where(mine, kind[k:k + 1], 0.0) for k in range(faces + 1)], axis=0
    ).astype(BF16)
    place = ones(iota((e_dev, lane), 0) % rep == iota((e_dev, lane), 1) // (lane // rep))
    code[...] = jnp.dot(tall, place, preferred_element_type=F32).astype(jnp.int32)

    n_agg = coarse_row.shape[1]
    numbers = coarse_row
    across = iota((devices, n_agg), 1)
    targets = [where_sum(columns[t] == across, numbers, 1) for t in range(touch)]
    owners = [target // rows_own for target in targets]
    spot = iota((devices, rows_own), 1)
    present = jnp.zeros((devices, rows_own), F32)
    for t in range(touch):
        here = jnp.where(owners[t] == dev, targets[t] - owners[t] * rows_own, -1)
        present = jnp.where(here == spot, 1.0, present)
    mates = ones(iota((devices, devices), 0) // n_dev == iota((devices, devices), 1) // n_dev)
    shared = jnp.dot(mates, present.astype(BF16), preferred_element_type=F32) > 0
    shared = jnp.where(shared, 1.0, 0.0)
    lower = ones(iota((rows_own, rows_own), 0) < iota((rows_own, rows_own), 1))
    order = jnp.dot(shared.astype(BF16), lower, preferred_element_type=F32)
    heads = where_sum(row % n_dev == 0, shared * (order + 1.0 + (row // n_dev * group_rows).astype(F32)), 0)
    tab[...] = jnp.zeros(tab.shape, jnp.int32)
    put(0, jnp.minimum(heads.astype(jnp.int32), rows_own) - 1)
    spots = jnp.sum(present * (order + 1.0), axis=1, keepdims=True).astype(jnp.int32) - 1
    peer = iota((devices, n_dev), 1) + grp * n_dev
    put(2, where_sum(peer == iota((devices, n_dev), 0), spots, 0))
    inverse = jnp.full((1, n_dev), touch, jnp.int32)
    for t in range(touch):
        own = where_sum(row == device, owners[t], 0)
        inverse = jnp.where(own == iota((1, n_dev), 1), t, inverse)
    put(1, inverse)


def kernel(
    n_grp, n_dev, halo, group_rows, rows_own, n_agg,
    a_ref, p_ref, packed,
    out_ref,
    near_v, own_v, near, own, code,
    a_buf, p_buf, pool, pack, turned, left, prod, same_sum, part_t, parts, inbox, flat,
    *rest,
):
    *gathered, a_sem, p_sem, t_sem, h_send, h_recv, x_send, x_recv, g_send, g_recv = rest
    grp = lax.axis_index("grp")
    dev = lax.axis_index("dev")
    e_dev, width_c, width_b = p_ref.shape
    n_k = a_ref.shape[1]
    touch, _, lane = same_sum.shape
    rep = lane // width_c
    sub = width_c // rep
    groups = e_dev // rep
    chunks = chunks_of(n_k)
    parted = a_sem.shape[0] - n_k + 1

    def a_copies(k):
        count = parted if k == 1 else 1
        size = e_dev // count
        return [
            pltpu.make_async_copy(
                a_ref.at[pl.ds(q * size, size), k], a_buf.at[k, pl.ds(q * size, size)], a_sem.at[place_of(k, n_k) + (q if k == 1 else parted - 1)]
            )
            for q in range(count)
        ]

    faces = n_k - 1
    nbr = packed[0:faces, 0:e_dev]
    nbr_agg = packed[8:8 + faces, 0:e_dev]
    touch_agg = packed[16:16 + touch, 0:n_grp * n_dev]
    slot = packed[24:25, 0:e_dev]
    coarse_row = packed[32:33, 0:n_agg]
    p_copy = pltpu.make_async_copy(p_ref, p_buf, p_sem.at[0])
    near_copy = pltpu.make_async_copy(near_v, near, t_sem.at[0])
    own_copy = pltpu.make_async_copy(own_v, own, t_sem.at[1])
    p_copy.start()

    barrier = pltpu.get_barrier_semaphore()
    for off in range(1, n_dev):
        pl.semaphore_signal(
            barrier, inc=1, device_id=(grp, lax.rem(dev + off, n_dev)), device_id_type=MESH
        )
    for off in range(1, n_grp):
        pl.semaphore_signal(
            barrier, inc=1, device_id=(lax.rem(grp + off, n_grp), dev), device_id_type=MESH
        )

    dirs = (
        (grp > 0, (grp - 1, dev)),
        (grp < n_grp - 1, (grp + 1, dev)),
        (dev > 0, (grp, dev - 1)),
        (dev < n_dev - 1, (grp, dev + 1)),
    )

    def halo_copy(d, target):
        back = d ^ 1
        return pltpu.make_async_remote_copy(
            src_ref=pack.at[pl.ds(d * halo, halo)],
            dst_ref=pool.at[pl.ds(e_dev + back * halo, halo)],
            send_sem=h_send.at[d],
            recv_sem=h_recv.at[back],
            device_id=target,
            device_id_type=MESH,
        )

    def tables_one():
        halo_tables(grp, dev, n_grp, n_dev, halo, nbr, near_v)
        near_copy.start()

    def tables_two():
        owner_tables(
            grp, dev, n_dev, group_rows, rows_own,
            nbr, nbr_agg, slot, touch_agg, coarse_row, own_v, code,
        )
        part_t[touch] = jnp.zeros(part_t.shape[1:], BF16)
        own_copy.start()

    def a_first():
        for copy in a_copies(1):
            copy.start()

    def p_wait():
        p_copy.wait()
        for k in list(range(2, n_k)) + [0]:
            for copy in a_copies(k):
                copy.start()

    def turn_p():
        turn = ones(
            iota((width_c, width_c), 1)
            == iota((width_c, width_c), 0) % sub * rep + iota((width_c, width_c), 0) // sub
        )

        @pl.loop(0, e_dev, unroll=e_dev)
        def _(e):
            turned[e] = jnp.dot(turn, p_buf[e], preferred_element_type=F32).astype(BF16)

    def halo_start():
        near_copy.wait()
        for j in range(4 * halo):
            pack[j] = p_buf[near[8 + j % halo, j // halo]]
        pool[0:e_dev] = p_buf[...]
        pl.semaphore_wait(barrier, n_dev + n_grp - 2)
        for d, (there, target) in enumerate(dirs):
            @pl.when(there)
            def _(d=d, target=target):
                halo_copy(d, target).start()

    def halo_wait():
        for d, (there, target) in enumerate(dirs):
            @pl.when(there)
            def _(d=d, target=target):
                halo_copy(d, target).wait_send()
                pltpu.make_async_remote_copy(
                    src_ref=pack.at[pl.ds(d * halo, halo)],
                    dst_ref=pool.at[pl.ds(e_dev + d * halo, halo)],
                    send_sem=h_send.at[d],
                    recv_sem=h_recv.at[d],
                    device_id=target,
                    device_id_type=MESH,
                ).wait_recv()

    def left_of(k):
        copies = a_copies(k)
        for q, copy in enumerate(copies):
            copy.wait()
            size = e_dev // len(copies)

            @pl.loop(q * size, (q + 1) * size, unroll=size)
            def _(e):
                rows = pl.ds(pl.multiple_of(e * width_c, width_c), width_c)
                left[k, rows, :] = jnp.dot(
                    turned[e], a_buf[k, e], preferred_element_type=F32
                ).astype(BF16)

    group_of_lane = iota((width_c, lane), 1) // width_c
    sub_lane = iota((sub, lane), 1) // width_c

    def squeeze(total):
        pieces = [total[j * sub:(j + 1) * sub] for j in range(rep)]
        out = None
        for s in range(rep):
            picked = pieces[s]
            for g in range(1, rep):
                picked = jnp.where(sub_lane == g, pieces[(g + s) % rep], picked)
            if s:
                picked = pltpu.roll(picked, s * width_c, 1)
            out = picked if out is None else out + picked
        return out

    def right_mm(k):
        @pl.loop(0, groups, unroll=groups)
        def _(g):
            if k:
                blocks = [pool[near[k - 1, g * rep + i]] for i in range(rep)]
            else:
                blocks = [p_buf[g * rep + i] for i in range(rep)]
            rows = pl.ds(pl.multiple_of(g * lane, lane), lane)
            full = lax.dot_general(
                left[k, rows, :], jnp.concatenate(blocks, axis=0),
                (((1,), (1,)), ((), ())), preferred_element_type=F32,
            )
            picked = full[0:width_c]
            for i in range(1, rep):
                picked = jnp.where(group_of_lane == i, full[i * width_c:(i + 1) * width_c], picked)
            prod[k % 2, g] = picked

    def right_sum(k):
        def masked(t):
            total = None
            for g in range(groups):
                at = k * groups + g
                term = jnp.where(code[at:at + 1, :] == t, prod[k % 2, g], 0.0)
                total = term if total is None else total + term
            return total

        for t in range(touch):
            together = masked(t + touch)
            if k != 1:
                together = same_sum[t] + together
            if k:
                same_sum[t] = together
            part_t[t] = squeeze(masked(t) if k else together).astype(BF16)
        p = place_of(k, n_k)
        for o in range(n_dev):
            parts[p, o] = part_t[own[1, o]]
        inbox[p, dev] = parts[p, dev]

    def part_copy(c, off):
        start, size = chunks[c]
        target = lax.rem(dev + off, n_dev)
        return pltpu.make_async_remote_copy(
            src_ref=parts.at[pl.ds(start, size), target],
            dst_ref=inbox.at[pl.ds(start, size), dev],
            send_sem=x_send.at[c],
            recv_sem=x_recv.at[c],
            device_id=(grp, target),
            device_id_type=MESH,
        )

    def part_all(c):
        start, size = chunks[c]
        return pltpu.make_async_remote_copy(
            src_ref=parts.at[pl.ds(start, size), pl.ds(0, n_dev - 1)],
            dst_ref=inbox.at[pl.ds(start, size), pl.ds(0, n_dev - 1)],
            send_sem=x_send.at[c],
            recv_sem=x_recv.at[c],
            device_id=(grp, lax.rem(dev + 1, n_dev)),
            device_id_type=MESH,
        )

    def row_copy(c, off):
        target = lax.rem(grp + off, n_grp)
        return pltpu.make_async_remote_copy(
            src_ref=gathered[c].at[pl.ds(grp * group_rows, group_rows)],
            dst_ref=gathered[c].at[pl.ds(grp * group_rows, group_rows)],
            send_sem=g_send.at[c],
            recv_sem=g_recv.at[c],
            device_id=(target, dev),
            device_id_type=MESH,
        )

    def row_all(c):
        return pltpu.make_async_remote_copy(
            src_ref=gathered[c].at[pl.ds(0, (n_grp - 1) * group_rows)],
            dst_ref=gathered[c].at[pl.ds(0, (n_grp - 1) * group_rows)],
            send_sem=g_send.at[c],
            recv_sem=g_recv.at[c],
            device_id=(lax.rem(grp + 1, n_grp), dev),
            device_id_type=MESH,
        )

    def exchange(c):
        for off in range(1, n_dev):
            part_copy(c, off).start()

    def collect(c):
        part_all(c).wait_recv()
        start, size = chunks[c]
        for j in range(group_rows):
            for i in range(size):
                total = jnp.zeros((sub, lane), F32)
                for d in range(n_dev):
                    member = jnp.where(own[2, d] == j, 1.0, 0.0).astype(F32)
                    total = total + inbox[start + i, d].astype(F32) * member
                gathered[c][grp * group_rows + j, i] = total.astype(BF16)
        for off in range(1, n_grp):
            row_copy(c, off).start()

    def put_rows(rows, i, k):
        @pl.loop(0, rows_own, unroll=8)
        def _(r):
            at = own[0, r]
            row = rows[jnp.maximum(at, 0), i].astype(F32)
            flat[pl.ds(pl.multiple_of(r * sub, sub), sub), :] = jnp.where(at >= 0, row, 0.0)

        for j in range(sub):
            out_ref[k, :, j * lane:(j + 1) * lane] = flat[pl.ds(j, rows_own, stride=sub), :].astype(BF16)

    def place(c):
        row_all(c).wait_recv()
        start, size = chunks[c]
        for i in range(size):
            put_rows(gathered[c], i, (start + i + 1) % n_k)

    def sent():
        for c in range(len(chunks)):
            part_all(c).wait_send()
            row_all(c).wait_send()

    tables_one()
    a_first()
    tables_two()
    p_wait()
    halo_start()
    turn_p()
    left_of(1)
    left_of(2)
    own_copy.wait()
    left_of(3)
    left_of(4)
    halo_wait()
    right_mm(1)
    right_sum(1)
    exchange(0)
    right_mm(2)
    right_sum(2)
    exchange(1)
    left_of(5)
    right_mm(3)
    right_sum(3)
    exchange(2)
    left_of(6)
    right_mm(4)
    right_sum(4)
    exchange(3)
    right_mm(5)
    right_sum(5)
    exchange(4)
    collect(0)
    right_mm(6)
    right_sum(6)
    exchange(5)
    collect(1)
    left_of(0)
    right_mm(0)
    right_sum(0)
    exchange(6)
    collect(2)
    collect(3)
    collect(4)
    collect(5)
    collect(6)
    place(0)
    place(1)
    place(2)
    place(3)
    place(4)
    place(5)
    place(6)
    sent()


def on_device(n_grp, n_dev, a_blocks, prolong_t, elem_slot, touch_agg, nbr, nbr_agg, coarse_row):
    e_dev, width_c, width_b = prolong_t.shape
    n_k = a_blocks.shape[1]
    touch = touch_agg.shape[1]
    halo = e_dev // EX
    half_y = EY // 2
    span_y = half_y + 1
    group_rows = (n_dev * half_y + 1 + half_y) // span_y
    rows_own = n_grp * group_rows
    assert touch <= n_dev
    lane = 128
    rep = lane // width_c
    sub = width_c // rep
    groups = e_dev // rep
    chunks = chunks_of(n_k)
    n_chunks = len(chunks)
    parted = 2
    hbm = pl.BlockSpec(memory_space=pltpu.HBM)
    vmem = pl.BlockSpec(memory_space=pltpu.VMEM)
    ints = [nbr.T, nbr_agg.T, touch_agg.T, elem_slot.reshape(1, e_dev), coarse_row.reshape(1, -1)]
    width = -(-max(x.shape[1] for x in ints) // lane) * lane
    packed = sum(
        jnp.pad(x, ((8 * i, 8 * (len(ints) - i) - x.shape[0]), (0, width - x.shape[1])))
        for i, x in enumerate(ints)
    )
    out = pl.pallas_call(
        functools.partial(kernel, n_grp, n_dev, halo, group_rows, rows_own, coarse_row.shape[0]),
        out_shape=jax.ShapeDtypeStruct((n_k, rows_own, width_c * width_c), BF16),
        in_specs=[hbm] * 2 + [vmem],
        out_specs=vmem,
        scratch_shapes=[
            pltpu.VMEM((16, lane), jnp.int32),
            pltpu.VMEM((8, lane), jnp.int32),
            pltpu.SMEM((16, lane), jnp.int32),
            pltpu.SMEM((8, lane), jnp.int32),
            pltpu.VMEM((n_k * groups, lane), jnp.int32),
            pltpu.VMEM((n_k, e_dev, width_b, width_b), BF16),
            pltpu.VMEM((e_dev, width_c, width_b), BF16),
            pltpu.VMEM((e_dev + 4 * halo, width_c, width_b), BF16),
            pltpu.VMEM((4 * halo, width_c, width_b), BF16),
            pltpu.VMEM((e_dev, width_c, width_b), BF16),
            pltpu.VMEM((n_k, e_dev * width_c, width_b), BF16),
            pltpu.VMEM((2, groups, width_c, lane), F32),
            pltpu.VMEM((touch, width_c, lane), F32),
            pltpu.VMEM((touch + 1, sub, lane), BF16),
            pltpu.VMEM((n_k, n_dev, sub, lane), BF16),
            pltpu.VMEM((n_k, n_dev, sub, lane), BF16),
            pltpu.VMEM((rows_own * sub, lane), F32),
        ] + [pltpu.VMEM((rows_own, size, sub, lane), BF16) for _, size in chunks] + [
            pltpu.SemaphoreType.DMA((n_k + parted - 1,)),
            pltpu.SemaphoreType.DMA((1,)),
            pltpu.SemaphoreType.DMA((2,)),
            pltpu.SemaphoreType.DMA((4,)),
            pltpu.SemaphoreType.DMA((4,)),
            pltpu.SemaphoreType.DMA((n_chunks,)),
            pltpu.SemaphoreType.DMA((n_chunks,)),
            pltpu.SemaphoreType.DMA((n_chunks,)),
            pltpu.SemaphoreType.DMA((n_chunks,)),
        ],
        compiler_params=pltpu.CompilerParams(
            collective_id=0, has_side_effects=True, vmem_limit_bytes=54656 * 1024
        ),
        name="galerkin",
    )(a_blocks, prolong_t, packed)
    return out.astype(F32).transpose(1, 0, 2)


def solution(mesh):
    in_specs = (
        P(("grp", "dev"), None, None, None),
        P(("grp", "dev"), None, None),
        P(("grp", "dev")),
        P(),
        P(("grp", "dev"), None),
        P(("grp", "dev"), None),
        P(),
    )
    out_specs = P("dev", None, None)
    return jax.shard_map(
        functools.partial(on_device, mesh.shape["grp"], mesh.shape["dev"]),
        mesh=mesh, in_specs=in_specs, out_specs=out_specs, check_vma=False,
    )
```

```python
import functools

import jax
import jax.numpy as jnp
from jax import lax
from jax.experimental import pallas as pl
from jax.experimental.pallas import tpu as pltpu
from jax.sharding import PartitionSpec as P

EX = 4
EY = 4
MESH = pl.DeviceIdType.MESH
F32 = jnp.float32
BF16 = jnp.bfloat16


def iota(shape, dim):
    return lax.broadcasted_iota(jnp.int32, shape, dim)


def where_sum(mask, value, axis):
    return jnp.sum(jnp.where(mask, value, 0), axis=axis, keepdims=True)


def ones(mask):
    return jnp.where(mask, 1.0, 0.0).astype(BF16)


def place_of(k, n_k):
    return (k + n_k - 1) % n_k


def early_of(n_k):
    return 2


def chunks_of(n_k):
    return [(p, 2) for p in range(early_of(n_k), n_k - 1, 2)] + [(n_k - 1, 1)]


def halo_tables(grp, dev, n_grp, n_dev, halo, nbr, tab):
    device = grp * n_dev + dev
    faces, e_dev = nbr.shape
    near = [
        jnp.where(grp > 0, device - n_dev, -2),
        jnp.where(grp < n_grp - 1, device + n_dev, -2),
        jnp.where(dev > 0, device - 1, -2),
        jnp.where(dev < n_dev - 1, device + 1, -2),
    ]
    ids = nbr
    source = jnp.where(ids >= 0, jnp.maximum(ids, 0) // e_dev, -1)
    local = ids - source * e_dev
    hits = [jnp.max(jnp.where(source == n, 1.0, 0.0), axis=0, keepdims=True) for n in near]
    below = ones(iota((e_dev, e_dev), 0) < iota((e_dev, e_dev), 1))
    rank = jnp.dot(
        jnp.concatenate(hits + hits, axis=0).astype(BF16), below, preferred_element_type=F32
    ).astype(jnp.int32)
    lanes = iota((halo, e_dev), 1)
    tab[...] = jnp.zeros(tab.shape, jnp.int32)
    for d in range(4):
        found = (rank[d:d + 1] == iota((halo, e_dev), 0)) & (hits[d] > 0)
        tab[8:8 + halo, d:d + 1] = where_sum(found, lanes, 1)
    index = iota((e_dev, e_dev), 0)
    where_from = [jnp.where(source[f:f + 1] == device, local[f:f + 1], 0) for f in range(faces)]
    for d in range(4):
        seen = jnp.zeros((e_dev, e_dev), jnp.int32)
        for f in range(faces):
            seen = jnp.where(ids[f:f + 1] == near[d] * e_dev + index, 1, seen)
        seen = jnp.max(seen, axis=1, keepdims=True)
        for f in range(faces):
            ahead = where_sum(index < local[f:f + 1], seen, 0)
            where_from[f] = jnp.where(
                source[f:f + 1] == near[d], e_dev + d * halo + ahead, where_from[f]
            )
    for f in range(faces):
        tab[f:f + 1, 0:e_dev] = where_from[f]


def owner_tables(
    grp, dev, n_dev, group_rows, rows_own,
    nbr, nbr_agg, slot, touch_agg, coarse_row, tab, code, spot_of,
):
    device = grp * n_dev + dev
    faces, e_dev = nbr.shape
    touch, devices = touch_agg.shape
    lane = code.shape[1]
    groups = code.shape[0] // (faces + 1)
    rep = e_dev // groups

    def put(row, value):
        tab[row:row + 1, 0:value.shape[1]] = value

    ids = nbr
    row = iota((devices, 1), 0)
    entries = touch_agg.T
    columns = [entries[:, t:t + 1] for t in range(touch)]
    slots = slot
    own_agg = jnp.zeros((1, e_dev), jnp.int32)
    for t in range(touch):
        own_agg = jnp.where(slots == t, where_sum(row == device, columns[t], 0), own_agg)
    valid = ids >= 0
    same = valid & (nbr_agg == own_agg)
    kind = jnp.where(same, slots + touch, jnp.where(valid, slots, -1))
    kind = jnp.concatenate([slots + touch, kind], axis=0).astype(F32)
    mine = iota((groups, e_dev), 1) // rep == iota((groups, e_dev), 0)
    tall = jnp.concatenate(
        [jnp.where(mine, kind[k:k + 1], 0.0) for k in range(faces + 1)], axis=0
    ).astype(BF16)
    place = ones(iota((e_dev, lane), 0) % rep == iota((e_dev, lane), 1) // (lane // rep))
    code[...] = jnp.dot(tall, place, preferred_element_type=F32).astype(jnp.int32)

    n_agg = coarse_row.shape[1]
    numbers = coarse_row
    across = iota((devices, n_agg), 1)
    targets = [where_sum(columns[t] == across, numbers, 1) for t in range(touch)]
    owners = [target // rows_own for target in targets]
    spot = iota((devices, rows_own), 1)
    present = jnp.zeros((devices, rows_own), F32)
    for t in range(touch):
        here = jnp.where(owners[t] == dev, targets[t] - owners[t] * rows_own, -1)
        present = jnp.where(here == spot, 1.0, present)
    mates = ones(iota((devices, devices), 0) // n_dev == iota((devices, devices), 1) // n_dev)
    shared = jnp.dot(mates, present.astype(BF16), preferred_element_type=F32) > 0
    shared = jnp.where(shared, 1.0, 0.0)
    lower = ones(iota((rows_own, rows_own), 0) < iota((rows_own, rows_own), 1))
    order = jnp.dot(shared.astype(BF16), lower, preferred_element_type=F32)
    heads = where_sum(row % n_dev == 0, shared * (order + 1.0 + (row // n_dev * group_rows).astype(F32)), 0)
    tab[...] = jnp.zeros(tab.shape, jnp.int32)
    put(0, jnp.minimum(heads.astype(jnp.int32), rows_own) - 1)
    spots = jnp.sum(present * (order + 1.0), axis=1, keepdims=True).astype(jnp.int32) - 1
    spot_of[...] = jnp.broadcast_to(spots, spot_of.shape)
    peer = iota((devices, n_dev), 1) + grp * n_dev
    put(2, where_sum(peer == iota((devices, n_dev), 0), spots, 0))
    inverse = jnp.full((1, n_dev), touch, jnp.int32)
    for t in range(touch):
        own = where_sum(row == device, owners[t], 0)
        inverse = jnp.where(own == iota((1, n_dev), 1), t, inverse)
    put(1, inverse)


def kernel(
    n_grp, n_dev, halo, group_rows, rows_own, n_agg,
    a_ref, p_ref, packed,
    out_ref,
    near_v, own_v, near, own, code,
    a_buf, p_buf, pool, tail, pack, tail_pack, tail_in, turned, left, prod, same_sum, part_t, parts, inbox, flat, spot_of, z_in, y_in, early_rows,
    *rest,
):
    *gathered, a_sem, p_sem, t_sem, h_send, h_recv, x_send, x_recv, g_send, g_recv, f_recv, z_sem, y_sem = rest
    grp = lax.axis_index("grp")
    dev = lax.axis_index("dev")
    e_dev, width_c, width_b = p_ref.shape
    n_k = a_ref.shape[1]
    touch, _, lane = same_sum.shape
    rep = lane // width_c
    sub = width_c // rep
    groups = e_dev // rep
    chunks = chunks_of(n_k)
    early = early_of(n_k)
    rest_b = width_b - lane
    parted = a_sem.shape[0] - n_k + 1

    def a_copies(k):
        count = parted if k == 1 else 1
        size = e_dev // count
        return [
            pltpu.make_async_copy(
                a_ref.at[pl.ds(q * size, size), k], a_buf.at[k, pl.ds(q * size, size)], a_sem.at[place_of(k, n_k) + (q if k == 1 else parted - 1)]
            )
            for q in range(count)
        ]

    faces = n_k - 1
    nbr = packed[0:faces, 0:e_dev]
    nbr_agg = packed[8:8 + faces, 0:e_dev]
    touch_agg = packed[16:16 + touch, 0:n_grp * n_dev]
    slot = packed[24:25, 0:e_dev]
    coarse_row = packed[32:33, 0:n_agg]
    p_copy = pltpu.make_async_copy(p_ref, p_buf, p_sem.at[0])
    near_copy = pltpu.make_async_copy(near_v, near, t_sem.at[0])
    own_copy = pltpu.make_async_copy(own_v, own, t_sem.at[1])
    p_copy.start()

    barrier = pltpu.get_barrier_semaphore()
    for off in range(1, n_dev):
        pl.semaphore_signal(
            barrier, inc=1, device_id=(grp, lax.rem(dev + off, n_dev)), device_id_type=MESH
        )
    for off in range(1, n_grp):
        pl.semaphore_signal(
            barrier, inc=1, device_id=(lax.rem(grp + off, n_grp), dev), device_id_type=MESH
        )

    dirs = (
        (grp > 0, (grp - 1, dev)),
        (grp < n_grp - 1, (grp + 1, dev)),
        (dev > 0, (grp, dev - 1)),
        (dev < n_dev - 1, (grp, dev + 1)),
    )

    def halo_copy(part, d, target, back):
        source, sink, base, size = ((pack, pool, e_dev, halo), (tail_pack, tail_in, 0, halo // 2))[part]
        return pltpu.make_async_remote_copy(
            src_ref=source.at[pl.ds(d * size, size)],
            dst_ref=sink.at[pl.ds(base + back * size, size)],
            send_sem=h_send.at[4 * part + d],
            recv_sem=h_recv.at[4 * part + back],
            device_id=target,
            device_id_type=MESH,
        )

    def tables_one():
        halo_tables(grp, dev, n_grp, n_dev, halo, nbr, near_v)
        near_copy.start()

    def tables_two():
        owner_tables(
            grp, dev, n_dev, group_rows, rows_own,
            nbr, nbr_agg, slot, touch_agg, coarse_row, own_v, code, spot_of,
        )
        part_t[touch] = jnp.zeros(part_t.shape[1:], BF16)
        own_copy.start()

    def a_first():
        for copy in a_copies(1):
            copy.start()

    def p_wait():
        p_copy.wait()
        for k in list(range(2, n_k)) + [0]:
            for copy in a_copies(k):
                copy.start()

    def turn_p():
        turn = ones(
            iota((width_c, width_c), 1)
            == iota((width_c, width_c), 0) % sub * rep + iota((width_c, width_c), 0) // sub
        )

        @pl.loop(0, e_dev, unroll=e_dev)
        def _(e):
            turned[e] = jnp.dot(turn, p_buf[e], preferred_element_type=F32).astype(BF16)

    def halo_start():
        near_copy.wait()
        def start(part):
            for d, (there, target) in enumerate(dirs):
                @pl.when(there)
                def _(d=d, target=target):
                    halo_copy(part, d, target, d ^ 1).start()

        for j in range(4 * halo):
            pack[j] = p_buf[near[8 + j % halo, j // halo], :, :lane]
        pl.semaphore_wait(barrier, n_dev + n_grp - 2)
        start(0)
        for j in range(0, 4 * halo, 2):
            first = p_buf[near[8 + j % halo, j // halo], :, lane:]
            second = p_buf[near[8 + j % halo + 1, j // halo], :, lane:]
            tail_pack[j // 2] = jnp.concatenate([first, second], axis=1)
        start(1)
        pool[0:e_dev] = p_buf[:, :, :lane]
        tail[0:e_dev] = p_buf[:, :, lane:]

    def halo_wait():
        for d, (there, target) in enumerate(dirs):
            @pl.when(there)
            def _(d=d, target=target):
                for part in range(2):
                    halo_copy(part, d, target, d ^ 1).wait_send()
                    halo_copy(part, d, target, d).wait_recv()
                for j in range(d * halo // 2, (d + 1) * halo // 2):
                    both = tail_in[j]
                    tail[e_dev + 2 * j] = both[:, :rest_b]
                    tail[e_dev + 2 * j + 1] = both[:, rest_b:]

    def left_of(k):
        @pl.loop(0, e_dev, unroll=e_dev)
        def _(e):
            rows = pl.ds(pl.multiple_of(e * width_c, width_c), width_c)
            left[k, rows, :] = jnp.dot(
                turned[e], a_buf[k, e], preferred_element_type=F32
            ).astype(BF16)

    def a_wait(*ks):
        for k in ks:
            for copy in a_copies(k):
                copy.wait()

    group_of_lane = iota((width_c, lane), 1) // width_c
    sub_lane = iota((sub, lane), 1) // width_c

    def squeeze(total):
        pieces = [total[j * sub:(j + 1) * sub] for j in range(rep)]
        out = None
        for s in range(rep):
            picked = pieces[s]
            for g in range(1, rep):
                picked = jnp.where(sub_lane == g, pieces[(g + s) % rep], picked)
            if s:
                picked = pltpu.roll(picked, s * width_c, 1)
            out = picked if out is None else out + picked
        return out

    def right_mm(k):
        @pl.loop(0, groups, unroll=groups)
        def _(g):
            if k:
                at = [near[k - 1, g * rep + i] for i in range(rep)]
                blocks = [jnp.concatenate([pool[i], tail[i]], axis=1) for i in at]
            else:
                blocks = [p_buf[g * rep + i] for i in range(rep)]
            rows = pl.ds(pl.multiple_of(g * lane, lane), lane)
            full = lax.dot_general(
                left[k, rows, :], jnp.concatenate(blocks, axis=0),
                (((1,), (1,)), ((), ())), preferred_element_type=F32,
            )
            picked = full[0:width_c]
            for i in range(1, rep):
                picked = jnp.where(group_of_lane == i, full[i * width_c:(i + 1) * width_c], picked)
            prod[k, g] = picked

    def right_sum(k):
        def masked(t):
            total = None
            for g in range(groups):
                at = k * groups + g
                term = jnp.where(code[at:at + 1, :] == t, prod[k, g], 0.0)
                total = term if total is None else total + term
            return total

        for t in range(touch):
            together = masked(t + touch)
            if k != 1:
                together = same_sum[t] + together
            if k:
                same_sum[t] = together
            part_t[t] = squeeze(masked(t) if k else together).astype(BF16)
        p = place_of(k, n_k)
        for o in range(n_dev):
            parts[p, o] = part_t[own[1, o]]
        if p < early:
            z_in[grp, p] = parts[p]
        else:
            inbox[p, dev] = parts[p, dev]

    def column_copy(p, off):
        return pltpu.make_async_remote_copy(
            src_ref=parts.at[p],
            dst_ref=z_in.at[grp, p],
            send_sem=z_sem.at[0],
            recv_sem=z_sem.at[1],
            device_id=(lax.rem(grp + off, n_grp), dev),
            device_id_type=MESH,
        )

    def column_all():
        others = z_in.at[pl.ds(0, n_grp - 1)]
        return pltpu.make_async_remote_copy(
            src_ref=others,
            dst_ref=others,
            send_sem=z_sem.at[0],
            recv_sem=z_sem.at[1],
            device_id=(lax.rem(grp + 1, n_grp), dev),
            device_id_type=MESH,
        )

    def column_start(p):
        for off in range(1, n_grp):
            column_copy(p, off).start()

    def plane_copy(off):
        target = lax.rem(dev + off, n_dev)
        return pltpu.make_async_remote_copy(
            src_ref=z_in.at[:, :, target],
            dst_ref=y_in.at[dev],
            send_sem=y_sem.at[0],
            recv_sem=y_sem.at[1],
            device_id=(grp, target),
            device_id_type=MESH,
        )

    def plane_all():
        others = y_in.at[pl.ds(0, n_dev - 1)]
        return pltpu.make_async_remote_copy(
            src_ref=others,
            dst_ref=others,
            send_sem=y_sem.at[0],
            recv_sem=y_sem.at[1],
            device_id=(grp, lax.rem(dev + 1, n_dev)),
            device_id_type=MESH,
        )

    def plane_start():
        column_all().wait_recv()
        y_in[dev] = z_in[:, :, dev]
        for off in range(1, n_dev):
            plane_copy(off).start()

    def early_place():
        plane_all().wait_recv()

        @pl.loop(0, n_grp, unroll=n_grp)
        def _(g):
            spots = [spot_of[pl.ds(g * n_dev + d, 1), :] for d in range(n_dev)]
            for p in range(early):
                values = [y_in[d, g, p].astype(F32) for d in range(n_dev)]
                for j in range(group_rows):
                    total = None
                    for d in range(n_dev):
                        term = jnp.where(spots[d] == j, values[d], 0.0)
                        total = term if total is None else total + term
                    early_rows[g * group_rows + j, p] = total.astype(BF16)

        for p in range(early):
            put_rows(early_rows, p, p + 1)

    def part_copy(c, off):
        start, size = chunks[c]
        target = lax.rem(dev + off, n_dev)
        return pltpu.make_async_remote_copy(
            src_ref=parts.at[pl.ds(start, size), target],
            dst_ref=inbox.at[pl.ds(start, size), dev],
            send_sem=x_send.at[c],
            recv_sem=x_recv.at[c],
            device_id=(grp, target),
            device_id_type=MESH,
        )

    def part_all(c):
        start, size = chunks[c]
        return pltpu.make_async_remote_copy(
            src_ref=parts.at[pl.ds(start, size), pl.ds(0, n_dev - 1)],
            dst_ref=inbox.at[pl.ds(start, size), pl.ds(0, n_dev - 1)],
            send_sem=x_send.at[c],
            recv_sem=x_recv.at[c],
            device_id=(grp, lax.rem(dev + 1, n_dev)),
            device_id_type=MESH,
        )

    def relayed(c):
        return n_grp == 4 and c < 1

    def block_of(c, sender):
        return gathered[c].at[pl.ds(sender * group_rows, group_rows)]

    def row_copy(c, sender, target, sem):
        return pltpu.make_async_remote_copy(
            src_ref=block_of(c, sender),
            dst_ref=block_of(c, sender),
            send_sem=g_send.at[c],
            recv_sem=sem,
            device_id=(target, dev),
            device_id_type=MESH,
        )

    def row_all(c, count):
        rows = gathered[c].at[pl.ds(0, count * group_rows)]
        return pltpu.make_async_remote_copy(
            src_ref=rows,
            dst_ref=rows,
            send_sem=g_send.at[c],
            recv_sem=g_recv.at[c],
            device_id=(lax.rem(grp + 1, n_grp), dev),
            device_id_type=MESH,
        )

    def send_rows(c):
        if not relayed(c):
            for off in range(1, n_grp):
                row_copy(c, grp, lax.rem(grp + off, n_grp), g_recv.at[c]).start()
            return
        for g in range(4):
            @pl.when(grp == g)
            def _(g=g):
                for target in sorted(range(4), key=lambda t: abs(t - g)):
                    if 0 < abs(target - g) < 3:
                        far = (g, target) in ((0, 2), (3, 1))
                        row_copy(c, g, target, f_recv.at[c] if far else g_recv.at[c]).start()

    def relay(c):
        for g, sender in ((1, 3), (2, 0)):
            @pl.when(grp == g)
            def _(g=g, sender=sender):
                row_copy(c, sender, g, f_recv.at[c]).wait_recv()
                row_copy(c, sender, 3 - sender, g_recv.at[c]).start()

    def rows_arrived(c):
        if not relayed(c):
            row_all(c, n_grp - 1).wait_recv()
            return
        inner = (grp == 1) | (grp == 2)

        @pl.when(inner)
        def _():
            row_all(c, 2).wait_recv()

        @pl.when(jnp.logical_not(inner))
        def _():
            row_all(c, 3).wait_recv()

    def rows_sent(c):
        if not relayed(c):
            row_all(c, n_grp - 1).wait_send()
            return
        inner = (grp == 1) | (grp == 2)

        @pl.when(inner)
        def _():
            row_all(c, 4).wait_send()

        @pl.when(jnp.logical_not(inner))
        def _():
            row_all(c, 2).wait_send()

    def exchange(c):
        for off in range(1, n_dev):
            part_copy(c, off).start()

    def collect(c):
        part_all(c).wait_recv()
        start, size = chunks[c]
        for j in range(group_rows):
            for i in range(size):
                total = jnp.zeros((sub, lane), F32)
                for d in range(n_dev):
                    member = jnp.where(own[2, d] == j, 1.0, 0.0).astype(F32)
                    total = total + inbox[start + i, d].astype(F32) * member
                gathered[c][grp * group_rows + j, i] = total.astype(BF16)
        send_rows(c)

    def put_rows(rows, i, k):
        @pl.loop(0, rows_own, unroll=8)
        def _(r):
            at = own[0, r]
            row = rows[jnp.maximum(at, 0), i].astype(F32)
            flat[pl.ds(pl.multiple_of(r * sub, sub), sub), :] = jnp.where(at >= 0, row, 0.0)

        for j in range(sub):
            out_ref[k, :, j * lane:(j + 1) * lane] = flat[pl.ds(j, rows_own, stride=sub), :].astype(BF16)

    def place(c):
        rows_arrived(c)
        start, size = chunks[c]
        for i in range(size):
            put_rows(gathered[c], i, (start + i + 1) % n_k)

    def sent():
        column_all().wait_send()
        plane_all().wait_send()
        for c in range(len(chunks)):
            part_all(c).wait_send()
            rows_sent(c)

    tables_one()
    a_first()
    tables_two()
    p_wait()
    halo_start()
    turn_p()
    a_wait(1)
    left_of(1)
    a_wait(2)
    left_of(2)
    own_copy.wait()
    a_wait(3)
    left_of(3)
    a_wait(4)
    left_of(4)
    halo_wait()
    right_mm(1)
    right_mm(2)
    right_mm(3)
    right_mm(4)
    right_sum(1)
    right_sum(2)
    right_sum(3)
    right_sum(4)
    column_start(0)
    column_start(1)
    exchange(0)
    a_wait(5,6)
    left_of(5)
    left_of(6)
    right_mm(5)
    right_mm(6)
    right_sum(5)
    right_sum(6)
    exchange(1)
    a_wait(0)
    left_of(0)
    right_mm(0)
    right_sum(0)
    exchange(2)
    collect(0)
    collect(1)
    collect(2)
    plane_start()
    relay(0)
    early_place()
    place(0)
    place(1)
    place(2)
    sent()


def on_device(n_grp, n_dev, a_blocks, prolong_t, elem_slot, touch_agg, nbr, nbr_agg, coarse_row):
    e_dev, width_c, width_b = prolong_t.shape
    n_k = a_blocks.shape[1]
    touch = touch_agg.shape[1]
    halo = e_dev // EX
    half_y = EY // 2
    span_y = half_y + 1
    group_rows = (n_dev * half_y + 1 + half_y) // span_y
    rows_own = n_grp * group_rows
    assert touch <= n_dev
    lane = 128
    rep = lane // width_c
    sub = width_c // rep
    groups = e_dev // rep
    chunks = chunks_of(n_k)
    n_chunks = len(chunks)
    early = early_of(n_k)
    parted = 1
    hbm = pl.BlockSpec(memory_space=pltpu.HBM)
    vmem = pl.BlockSpec(memory_space=pltpu.VMEM)
    ints = [nbr.T, nbr_agg.T, touch_agg.T, elem_slot.reshape(1, e_dev), coarse_row.reshape(1, -1)]
    width = -(-max(x.shape[1] for x in ints) // lane) * lane
    packed = sum(
        jnp.pad(x, ((8 * i, 8 * (len(ints) - i) - x.shape[0]), (0, width - x.shape[1])))
        for i, x in enumerate(ints)
    )
    out = pl.pallas_call(
        functools.partial(kernel, n_grp, n_dev, halo, group_rows, rows_own, coarse_row.shape[0]),
        out_shape=jax.ShapeDtypeStruct((n_k, rows_own, width_c * width_c), BF16),
        in_specs=[hbm] * 2 + [vmem],
        out_specs=vmem,
        scratch_shapes=[
            pltpu.VMEM((16, lane), jnp.int32),
            pltpu.VMEM((8, lane), jnp.int32),
            pltpu.SMEM((16, lane), jnp.int32),
            pltpu.SMEM((8, lane), jnp.int32),
            pltpu.VMEM((n_k * groups, lane), jnp.int32),
            pltpu.VMEM((n_k, e_dev, width_b, width_b), BF16),
            pltpu.VMEM((e_dev, width_c, width_b), BF16),
            pltpu.VMEM((e_dev + 4 * halo, width_c, lane), BF16),
            pltpu.VMEM((e_dev + 4 * halo, width_c, width_b - lane), BF16),
            pltpu.VMEM((4 * halo, width_c, lane), BF16),
            pltpu.VMEM((2 * halo, width_c, lane), BF16),
            pltpu.VMEM((2 * halo, width_c, lane), BF16),
            pltpu.VMEM((e_dev, width_c, width_b), BF16),
            pltpu.VMEM((n_k, e_dev * width_c, width_b), BF16),
            pltpu.VMEM((n_k, groups, width_c, lane), F32),
            pltpu.VMEM((touch, width_c, lane), F32),
            pltpu.VMEM((touch + 1, sub, lane), BF16),
            pltpu.VMEM((n_k, n_dev, sub, lane), BF16),
            pltpu.VMEM((n_k, n_dev, sub, lane), BF16),
            pltpu.VMEM((rows_own * sub, lane), F32),
            pltpu.VMEM((n_grp * n_dev, lane), jnp.int32),
            pltpu.VMEM((n_grp, early, n_dev, sub, lane), BF16),
            pltpu.VMEM((n_dev, n_grp, early, sub, lane), BF16),
            pltpu.VMEM((rows_own, early, sub, lane), BF16),
        ] + [pltpu.VMEM((rows_own, size, sub, lane), BF16) for _, size in chunks] + [
            pltpu.SemaphoreType.DMA((n_k + parted - 1,)),
            pltpu.SemaphoreType.DMA((1,)),
            pltpu.SemaphoreType.DMA((2,)),
            pltpu.SemaphoreType.DMA((8,)),
            pltpu.SemaphoreType.DMA((8,)),
            pltpu.SemaphoreType.DMA((n_chunks,)),
            pltpu.SemaphoreType.DMA((n_chunks,)),
            pltpu.SemaphoreType.DMA((n_chunks,)),
            pltpu.SemaphoreType.DMA((n_chunks,)),
            pltpu.SemaphoreType.DMA((n_chunks,)),
            pltpu.SemaphoreType.DMA((2,)),
            pltpu.SemaphoreType.DMA((2,)),
        ],
        compiler_params=pltpu.CompilerParams(
            collective_id=0, has_side_effects=True, vmem_limit_bytes=54656 * 1024
        ),
        name="galerkin",
    )(a_blocks, prolong_t, packed)
    return out.astype(F32).transpose(1, 0, 2)


def solution(mesh):
    in_specs = (
        P(("grp", "dev"), None, None, None),
        P(("grp", "dev"), None, None),
        P(("grp", "dev")),
        P(),
        P(("grp", "dev"), None),
        P(("grp", "dev"), None),
        P(),
    )
    out_specs = P("dev", None, None)
    return jax.shard_map(
        functools.partial(on_device, mesh.shape["grp"], mesh.shape["dev"]),
        mesh=mesh, in_specs=in_specs, out_specs=out_specs, check_vma=False,
    )
```

```python
import functools

import jax
import jax.numpy as jnp
from jax import lax
from jax.experimental import pallas as pl
from jax.experimental.pallas import tpu as pltpu
from jax.sharding import PartitionSpec as P

EX = 4
EY = 4
MESH = pl.DeviceIdType.MESH
F32 = jnp.float32
BF16 = jnp.bfloat16


def iota(shape, dim):
    return lax.broadcasted_iota(jnp.int32, shape, dim)


def where_sum(mask, value, axis):
    return jnp.sum(jnp.where(mask, value, 0), axis=axis, keepdims=True)


def ones(mask):
    return jnp.where(mask, 1.0, 0.0).astype(BF16)


def place_of(k, n_k):
    return (k + n_k - 1) % n_k


def early_of(n_k):
    return 2


def chunks_of(n_k):
    return [(p, 2) for p in range(early_of(n_k), n_k - 1, 2)] + [(n_k - 1, 1)]


def halo_tables(grp, dev, n_grp, n_dev, halo, nbr, tab):
    device = grp * n_dev + dev
    faces, e_dev = nbr.shape
    near = [
        jnp.where(grp > 0, device - n_dev, -2),
        jnp.where(grp < n_grp - 1, device + n_dev, -2),
        jnp.where(dev > 0, device - 1, -2),
        jnp.where(dev < n_dev - 1, device + 1, -2),
    ]
    ids = nbr
    source = jnp.where(ids >= 0, jnp.maximum(ids, 0) // e_dev, -1)
    local = ids - source * e_dev
    hits = [jnp.max(jnp.where(source == n, 1.0, 0.0), axis=0, keepdims=True) for n in near]
    below = ones(iota((e_dev, e_dev), 0) < iota((e_dev, e_dev), 1))
    rank = jnp.dot(
        jnp.concatenate(hits + hits, axis=0).astype(BF16), below, preferred_element_type=F32
    ).astype(jnp.int32)
    lanes = iota((halo, e_dev), 1)
    tab[...] = jnp.zeros(tab.shape, jnp.int32)
    for d in range(4):
        found = (rank[d:d + 1] == iota((halo, e_dev), 0)) & (hits[d] > 0)
        tab[8:8 + halo, d:d + 1] = where_sum(found, lanes, 1)
    index = iota((e_dev, e_dev), 0)
    where_from = [jnp.where(source[f:f + 1] == device, local[f:f + 1], 0) for f in range(faces)]
    for d in range(4):
        seen = jnp.zeros((e_dev, e_dev), jnp.int32)
        for f in range(faces):
            seen = jnp.where(ids[f:f + 1] == near[d] * e_dev + index, 1, seen)
        seen = jnp.max(seen, axis=1, keepdims=True)
        for f in range(faces):
            ahead = where_sum(index < local[f:f + 1], seen, 0)
            where_from[f] = jnp.where(
                source[f:f + 1] == near[d], e_dev + d * halo + ahead, where_from[f]
            )
    for f in range(faces):
        tab[f:f + 1, 0:e_dev] = where_from[f]


def owner_tables(
    grp, dev, n_dev, group_rows, rows_own,
    nbr, nbr_agg, slot, touch_agg, coarse_row, tab, code, spot_of,
):
    device = grp * n_dev + dev
    faces, e_dev = nbr.shape
    touch, devices = touch_agg.shape
    lane = code.shape[1]
    groups = code.shape[0] // (faces + 1)
    rep = e_dev // groups

    def put(row, value):
        tab[row:row + 1, 0:value.shape[1]] = value

    ids = nbr
    row = iota((devices, 1), 0)
    entries = touch_agg.T
    columns = [entries[:, t:t + 1] for t in range(touch)]
    slots = slot
    own_agg = jnp.zeros((1, e_dev), jnp.int32)
    for t in range(touch):
        own_agg = jnp.where(slots == t, where_sum(row == device, columns[t], 0), own_agg)
    valid = ids >= 0
    same = valid & (nbr_agg == own_agg)
    kind = jnp.where(same, slots + touch, jnp.where(valid, slots, -1))
    kind = jnp.concatenate([slots + touch, kind], axis=0).astype(F32)
    mine = iota((groups, e_dev), 1) // rep == iota((groups, e_dev), 0)
    tall = jnp.concatenate(
        [jnp.where(mine, kind[k:k + 1], 0.0) for k in range(faces + 1)], axis=0
    ).astype(BF16)
    place = ones(iota((e_dev, lane), 0) % rep == iota((e_dev, lane), 1) // (lane // rep))
    code[...] = jnp.dot(tall, place, preferred_element_type=F32).astype(jnp.int32)

    n_agg = coarse_row.shape[1]
    numbers = coarse_row
    across = iota((devices, n_agg), 1)
    targets = [where_sum(columns[t] == across, numbers, 1) for t in range(touch)]
    owners = [target // rows_own for target in targets]
    spot = iota((devices, rows_own), 1)
    present = jnp.zeros((devices, rows_own), F32)
    for t in range(touch):
        here = jnp.where(owners[t] == dev, targets[t] - owners[t] * rows_own, -1)
        present = jnp.where(here == spot, 1.0, present)
    mates = ones(iota((devices, devices), 0) // n_dev == iota((devices, devices), 1) // n_dev)
    shared = jnp.dot(mates, present.astype(BF16), preferred_element_type=F32) > 0
    shared = jnp.where(shared, 1.0, 0.0)
    lower = ones(iota((rows_own, rows_own), 0) < iota((rows_own, rows_own), 1))
    order = jnp.dot(shared.astype(BF16), lower, preferred_element_type=F32)
    heads = where_sum(row % n_dev == 0, shared * (order + 1.0 + (row // n_dev * group_rows).astype(F32)), 0)
    tab[...] = jnp.zeros(tab.shape, jnp.int32)
    put(0, jnp.minimum(heads.astype(jnp.int32), rows_own) - 1)
    spots = jnp.sum(present * (order + 1.0), axis=1, keepdims=True).astype(jnp.int32) - 1
    spot_of[...] = jnp.broadcast_to(spots, spot_of.shape)
    peer = iota((devices, n_dev), 1) + grp * n_dev
    put(2, where_sum(peer == iota((devices, n_dev), 0), spots, 0))
    inverse = jnp.full((1, n_dev), touch, jnp.int32)
    for t in range(touch):
        own = where_sum(row == device, owners[t], 0)
        inverse = jnp.where(own == iota((1, n_dev), 1), t, inverse)
    put(1, inverse)


def kernel(
    n_grp, n_dev, halo, group_rows, rows_own, n_agg,
    a_ref, p_ref, packed,
    out_ref,
    near_v, own_v, near, own, code,
    a_buf, p_buf, pool, tail, pack, tail_pack, tail_in, turned, left, prod, same_sum, part_t, parts, inbox, flat, spot_of, z_in, y_in, early_rows,
    *rest,
):
    *gathered, a_sem, p_sem, t_sem, h_send, h_recv, x_send, x_recv, g_send, g_recv, f_recv, z_sem, y_sem = rest
    grp = lax.axis_index("grp")
    dev = lax.axis_index("dev")
    e_dev, width_c, width_b = p_ref.shape
    n_k = a_ref.shape[1]
    touch, _, lane = same_sum.shape
    rep = lane // width_c
    sub = width_c // rep
    groups = e_dev // rep
    chunks = chunks_of(n_k)
    early = early_of(n_k)
    rest_b = width_b - lane
    parted = a_sem.shape[0] - n_k + 1

    def a_copies(k):
        count = parted if k == 0 else 1
        size = e_dev // count
        return [
            pltpu.make_async_copy(
                a_ref.at[pl.ds(q * size, size), k], a_buf.at[k, pl.ds(q * size, size)], a_sem.at[place_of(k, n_k) + q]
            )
            for q in range(count)
        ]

    faces = n_k - 1
    nbr = packed[0:faces, 0:e_dev]
    nbr_agg = packed[8:8 + faces, 0:e_dev]
    touch_agg = packed[16:16 + touch, 0:n_grp * n_dev]
    slot = packed[24:25, 0:e_dev]
    coarse_row = packed[32:33, 0:n_agg]
    p_copy = pltpu.make_async_copy(p_ref, p_buf, p_sem.at[0])
    near_copy = pltpu.make_async_copy(near_v, near, t_sem.at[0])
    own_copy = pltpu.make_async_copy(own_v, own, t_sem.at[1])
    p_copy.start()

    barrier = pltpu.get_barrier_semaphore()
    for off in range(1, n_dev):
        pl.semaphore_signal(
            barrier, inc=1, device_id=(grp, lax.rem(dev + off, n_dev)), device_id_type=MESH
        )
    for off in range(1, n_grp):
        pl.semaphore_signal(
            barrier, inc=1, device_id=(lax.rem(grp + off, n_grp), dev), device_id_type=MESH
        )

    dirs = (
        (grp > 0, (grp - 1, dev)),
        (grp < n_grp - 1, (grp + 1, dev)),
        (dev > 0, (grp, dev - 1)),
        (dev < n_dev - 1, (grp, dev + 1)),
    )

    def halo_copy(part, d, target, back):
        source, sink, base, size = ((pack, pool, e_dev, halo), (tail_pack, tail_in, 0, halo // 2))[part]
        return pltpu.make_async_remote_copy(
            src_ref=source.at[pl.ds(d * size, size)],
            dst_ref=sink.at[pl.ds(base + back * size, size)],
            send_sem=h_send.at[4 * part + d],
            recv_sem=h_recv.at[4 * part + back],
            device_id=target,
            device_id_type=MESH,
        )

    def tables_one():
        halo_tables(grp, dev, n_grp, n_dev, halo, nbr, near_v)
        near_copy.start()

    def tables_two():
        owner_tables(
            grp, dev, n_dev, group_rows, rows_own,
            nbr, nbr_agg, slot, touch_agg, coarse_row, own_v, code, spot_of,
        )
        part_t[touch] = jnp.zeros(part_t.shape[1:], BF16)
        own_copy.start()

    def a_first():
        for copy in a_copies(1):
            copy.start()

    def p_wait():
        p_copy.wait()
        for k in list(range(2, n_k)) + [0]:
            for copy in a_copies(k):
                copy.start()

    def turn_p():
        turn = ones(
            iota((width_c, width_c), 1)
            == iota((width_c, width_c), 0) % sub * rep + iota((width_c, width_c), 0) // sub
        )

        @pl.loop(0, e_dev, unroll=e_dev)
        def _(e):
            turned[e] = jnp.dot(turn, p_buf[e], preferred_element_type=F32).astype(BF16)

    def halo_start():
        near_copy.wait()
        def start(part):
            for d, (there, target) in enumerate(dirs):
                @pl.when(there)
                def _(d=d, target=target):
                    halo_copy(part, d, target, d ^ 1).start()

        for j in range(4 * halo):
            pack[j] = p_buf[near[8 + j % halo, j // halo], :, :lane]
        pl.semaphore_wait(barrier, n_dev + n_grp - 2)
        start(0)
        for j in range(0, 4 * halo, 2):
            first = p_buf[near[8 + j % halo, j // halo], :, lane:]
            second = p_buf[near[8 + j % halo + 1, j // halo], :, lane:]
            tail_pack[j // 2] = jnp.concatenate([first, second], axis=1)
        start(1)
        pool[0:e_dev] = p_buf[:, :, :lane]
        tail[0:e_dev] = p_buf[:, :, lane:]

    def halo_wait():
        for d, (there, target) in enumerate(dirs):
            @pl.when(there)
            def _(d=d, target=target):
                for part in range(2):
                    halo_copy(part, d, target, d ^ 1).wait_send()
                    halo_copy(part, d, target, d).wait_recv()
                for j in range(d * halo // 2, (d + 1) * halo // 2):
                    both = tail_in[j]
                    tail[e_dev + 2 * j] = both[:, :rest_b]
                    tail[e_dev + 2 * j + 1] = both[:, rest_b:]

    def left_of(k, part=0, count=1):
        size = e_dev // count

        @pl.loop(part * size, (part + 1) * size, unroll=size)
        def _(e):
            rows = pl.ds(pl.multiple_of(e * width_c, width_c), width_c)
            left[k, rows, :] = jnp.dot(
                turned[e], a_buf[k, e], preferred_element_type=F32
            ).astype(BF16)

    def a_wait(*ks):
        for k in ks:
            for copy in a_copies(k):
                copy.wait()

    group_of_lane = iota((width_c, lane), 1) // width_c
    sub_lane = iota((sub, lane), 1) // width_c

    def squeeze(total):
        pieces = [total[j * sub:(j + 1) * sub] for j in range(rep)]
        out = None
        for s in range(rep):
            picked = pieces[s]
            for g in range(1, rep):
                picked = jnp.where(sub_lane == g, pieces[(g + s) % rep], picked)
            if s:
                picked = pltpu.roll(picked, s * width_c, 1)
            out = picked if out is None else out + picked
        return out

    def right_mm(k, part=0, count=1):
        size = groups // count

        @pl.loop(part * size, (part + 1) * size, unroll=size)
        def _(g):
            if k:
                at = [near[k - 1, g * rep + i] for i in range(rep)]
                blocks = [jnp.concatenate([pool[i], tail[i]], axis=1) for i in at]
            else:
                blocks = [p_buf[g * rep + i] for i in range(rep)]
            rows = pl.ds(pl.multiple_of(g * lane, lane), lane)
            full = lax.dot_general(
                left[k, rows, :], jnp.concatenate(blocks, axis=0),
                (((1,), (1,)), ((), ())), preferred_element_type=F32,
            )
            picked = full[0:width_c]
            for i in range(1, rep):
                picked = jnp.where(group_of_lane == i, full[i * width_c:(i + 1) * width_c], picked)
            prod[k, g] = picked

    def own_last():
        for q, copy in enumerate(a_copies(0)):
            copy.wait()
            left_of(0, q, parted)
            right_mm(0, q, parted)

    def right_sum(k):
        def masked(t):
            total = None
            for g in range(groups):
                at = k * groups + g
                term = jnp.where(code[at:at + 1, :] == t, prod[k, g], 0.0)
                total = term if total is None else total + term
            return total

        for t in range(touch):
            together = masked(t + touch)
            if k != 1:
                together = same_sum[t] + together
            if k:
                same_sum[t] = together
            part_t[t] = squeeze(masked(t) if k else together).astype(BF16)
        p = place_of(k, n_k)
        for o in range(n_dev):
            parts[p, o] = part_t[own[1, o]]
        if p < early:
            z_in[grp, p] = parts[p]
        else:
            inbox[p, dev] = parts[p, dev]

    def column_copy(p, off):
        return pltpu.make_async_remote_copy(
            src_ref=parts.at[p],
            dst_ref=z_in.at[grp, p],
            send_sem=z_sem.at[0],
            recv_sem=z_sem.at[1],
            device_id=(lax.rem(grp + off, n_grp), dev),
            device_id_type=MESH,
        )

    def column_all():
        others = z_in.at[pl.ds(0, n_grp - 1)]
        return pltpu.make_async_remote_copy(
            src_ref=others,
            dst_ref=others,
            send_sem=z_sem.at[0],
            recv_sem=z_sem.at[1],
            device_id=(lax.rem(grp + 1, n_grp), dev),
            device_id_type=MESH,
        )

    def column_start(p):
        for off in range(1, n_grp):
            column_copy(p, off).start()

    def plane_copy(off):
        target = lax.rem(dev + off, n_dev)
        return pltpu.make_async_remote_copy(
            src_ref=z_in.at[:, :, target],
            dst_ref=y_in.at[dev],
            send_sem=y_sem.at[0],
            recv_sem=y_sem.at[1],
            device_id=(grp, target),
            device_id_type=MESH,
        )

    def plane_all():
        others = y_in.at[pl.ds(0, n_dev - 1)]
        return pltpu.make_async_remote_copy(
            src_ref=others,
            dst_ref=others,
            send_sem=y_sem.at[0],
            recv_sem=y_sem.at[1],
            device_id=(grp, lax.rem(dev + 1, n_dev)),
            device_id_type=MESH,
        )

    def plane_start():
        column_all().wait_recv()
        y_in[dev] = z_in[:, :, dev]
        for off in range(1, n_dev):
            plane_copy(off).start()

    def early_place():
        plane_all().wait_recv()

        @pl.loop(0, n_grp, unroll=n_grp)
        def _(g):
            spots = [spot_of[pl.ds(g * n_dev + d, 1), :] for d in range(n_dev)]
            for p in range(early):
                values = [y_in[d, g, p].astype(F32) for d in range(n_dev)]
                for j in range(group_rows):
                    total = None
                    for d in range(n_dev):
                        term = jnp.where(spots[d] == j, values[d], 0.0)
                        total = term if total is None else total + term
                    early_rows[g * group_rows + j, p] = total.astype(BF16)

        for p in range(early):
            put_rows(early_rows, p, p + 1)

    def part_copy(c, off):
        start, size = chunks[c]
        target = lax.rem(dev + off, n_dev)
        return pltpu.make_async_remote_copy(
            src_ref=parts.at[pl.ds(start, size), target],
            dst_ref=inbox.at[pl.ds(start, size), dev],
            send_sem=x_send.at[c],
            recv_sem=x_recv.at[c],
            device_id=(grp, target),
            device_id_type=MESH,
        )

    def part_all(c):
        start, size = chunks[c]
        return pltpu.make_async_remote_copy(
            src_ref=parts.at[pl.ds(start, size), pl.ds(0, n_dev - 1)],
            dst_ref=inbox.at[pl.ds(start, size), pl.ds(0, n_dev - 1)],
            send_sem=x_send.at[c],
            recv_sem=x_recv.at[c],
            device_id=(grp, lax.rem(dev + 1, n_dev)),
            device_id_type=MESH,
        )

    def relayed(c):
        return n_grp == 4 and c < 1

    def block_of(c, sender):
        return gathered[c].at[pl.ds(sender * group_rows, group_rows)]

    def row_copy(c, sender, target, sem):
        return pltpu.make_async_remote_copy(
            src_ref=block_of(c, sender),
            dst_ref=block_of(c, sender),
            send_sem=g_send.at[c],
            recv_sem=sem,
            device_id=(target, dev),
            device_id_type=MESH,
        )

    def row_all(c, count):
        rows = gathered[c].at[pl.ds(0, count * group_rows)]
        return pltpu.make_async_remote_copy(
            src_ref=rows,
            dst_ref=rows,
            send_sem=g_send.at[c],
            recv_sem=g_recv.at[c],
            device_id=(lax.rem(grp + 1, n_grp), dev),
            device_id_type=MESH,
        )

    def send_rows(c):
        if not relayed(c):
            for off in range(1, n_grp):
                row_copy(c, grp, lax.rem(grp + off, n_grp), g_recv.at[c]).start()
            return
        for g in range(4):
            @pl.when(grp == g)
            def _(g=g):
                for target in sorted(range(4), key=lambda t: abs(t - g)):
                    if 0 < abs(target - g) < 3:
                        far = (g, target) in ((0, 2), (3, 1))
                        row_copy(c, g, target, f_recv.at[c] if far else g_recv.at[c]).start()

    def relay(c):
        for g, sender in ((1, 3), (2, 0)):
            @pl.when(grp == g)
            def _(g=g, sender=sender):
                row_copy(c, sender, g, f_recv.at[c]).wait_recv()
                row_copy(c, sender, 3 - sender, g_recv.at[c]).start()

    def rows_arrived(c):
        if not relayed(c):
            row_all(c, n_grp - 1).wait_recv()
            return
        inner = (grp == 1) | (grp == 2)

        @pl.when(inner)
        def _():
            row_all(c, 2).wait_recv()

        @pl.when(jnp.logical_not(inner))
        def _():
            row_all(c, 3).wait_recv()

    def rows_sent(c):
        if not relayed(c):
            row_all(c, n_grp - 1).wait_send()
            return
        inner = (grp == 1) | (grp == 2)

        @pl.when(inner)
        def _():
            row_all(c, 4).wait_send()

        @pl.when(jnp.logical_not(inner))
        def _():
            row_all(c, 2).wait_send()

    def exchange(c):
        for off in range(1, n_dev):
            part_copy(c, off).start()

    def collect(c):
        part_all(c).wait_recv()
        start, size = chunks[c]
        for j in range(group_rows):
            for i in range(size):
                total = jnp.zeros((sub, lane), F32)
                for d in range(n_dev):
                    member = jnp.where(own[2, d] == j, 1.0, 0.0).astype(F32)
                    total = total + inbox[start + i, d].astype(F32) * member
                gathered[c][grp * group_rows + j, i] = total.astype(BF16)
        send_rows(c)

    def put_rows(rows, i, k):
        @pl.loop(0, rows_own, unroll=8)
        def _(r):
            at = own[0, r]
            row = rows[jnp.maximum(at, 0), i].astype(F32)
            flat[pl.ds(pl.multiple_of(r * sub, sub), sub), :] = jnp.where(at >= 0, row, 0.0)

        for j in range(sub):
            out_ref[k, :, j * lane:(j + 1) * lane] = flat[pl.ds(j, rows_own, stride=sub), :].astype(BF16)

    def place(c):
        rows_arrived(c)
        start, size = chunks[c]
        for i in range(size):
            put_rows(gathered[c], i, (start + i + 1) % n_k)

    def sent():
        column_all().wait_send()
        plane_all().wait_send()
        for c in range(len(chunks)):
            part_all(c).wait_send()
            rows_sent(c)

    tables_one()
    a_first()
    tables_two()
    p_wait()
    halo_start()
    turn_p()
    a_wait(1)
    left_of(1)
    a_wait(2)
    left_of(2)
    own_copy.wait()
    a_wait(3)
    left_of(3)
    a_wait(4)
    left_of(4)
    halo_wait()
    right_mm(1)
    right_mm(2)
    right_mm(3)
    right_mm(4)
    right_sum(1)
    right_sum(2)
    right_sum(3)
    right_sum(4)
    exchange(0)
    column_start(0)
    column_start(1)
    a_wait(5,6)
    left_of(5)
    left_of(6)
    right_mm(5)
    right_mm(6)
    right_sum(5)
    right_sum(6)
    exchange(1)
    a_wait(0)
    left_of(0)
    right_mm(0)
    right_sum(0)
    exchange(2)
    collect(0)
    plane_start()
    collect(1)
    collect(2)
    relay(0)
    early_place()
    place(1)
    place(2)
    place(0)
    sent()


def on_device(n_grp, n_dev, a_blocks, prolong_t, elem_slot, touch_agg, nbr, nbr_agg, coarse_row):
    e_dev, width_c, width_b = prolong_t.shape
    n_k = a_blocks.shape[1]
    touch = touch_agg.shape[1]
    halo = e_dev // EX
    half_y = EY // 2
    span_y = half_y + 1
    group_rows = (n_dev * half_y + 1 + half_y) // span_y
    rows_own = n_grp * group_rows
    assert touch <= n_dev
    lane = 128
    rep = lane // width_c
    sub = width_c // rep
    groups = e_dev // rep
    chunks = chunks_of(n_k)
    n_chunks = len(chunks)
    early = early_of(n_k)
    parted = 1
    hbm = pl.BlockSpec(memory_space=pltpu.HBM)
    vmem = pl.BlockSpec(memory_space=pltpu.VMEM)
    ints = [nbr.T, nbr_agg.T, touch_agg.T, elem_slot.reshape(1, e_dev), coarse_row.reshape(1, -1)]
    width = -(-max(x.shape[1] for x in ints) // lane) * lane
    packed = sum(
        jnp.pad(x, ((8 * i, 8 * (len(ints) - i) - x.shape[0]), (0, width - x.shape[1])))
        for i, x in enumerate(ints)
    )
    out = pl.pallas_call(
        functools.partial(kernel, n_grp, n_dev, halo, group_rows, rows_own, coarse_row.shape[0]),
        out_shape=jax.ShapeDtypeStruct((n_k, rows_own, width_c * width_c), BF16),
        in_specs=[hbm] * 2 + [vmem],
        out_specs=vmem,
        scratch_shapes=[
            pltpu.VMEM((16, lane), jnp.int32),
            pltpu.VMEM((8, lane), jnp.int32),
            pltpu.SMEM((16, lane), jnp.int32),
            pltpu.SMEM((8, lane), jnp.int32),
            pltpu.VMEM((n_k * groups, lane), jnp.int32),
            pltpu.VMEM((n_k, e_dev, width_b, width_b), BF16),
            pltpu.VMEM((e_dev, width_c, width_b), BF16),
            pltpu.VMEM((e_dev + 4 * halo, width_c, lane), BF16),
            pltpu.VMEM((e_dev + 4 * halo, width_c, width_b - lane), BF16),
            pltpu.VMEM((4 * halo, width_c, lane), BF16),
            pltpu.VMEM((2 * halo, width_c, lane), BF16),
            pltpu.VMEM((2 * halo, width_c, lane), BF16),
            pltpu.VMEM((e_dev, width_c, width_b), BF16),
            pltpu.VMEM((n_k, e_dev * width_c, width_b), BF16),
            pltpu.VMEM((n_k, groups, width_c, lane), F32),
            pltpu.VMEM((touch, width_c, lane), F32),
            pltpu.VMEM((touch + 1, sub, lane), BF16),
            pltpu.VMEM((n_k, n_dev, sub, lane), BF16),
            pltpu.VMEM((n_k, n_dev, sub, lane), BF16),
            pltpu.VMEM((rows_own * sub, lane), F32),
            pltpu.VMEM((n_grp * n_dev, lane), jnp.int32),
            pltpu.VMEM((n_grp, early, n_dev, sub, lane), BF16),
            pltpu.VMEM((n_dev, n_grp, early, sub, lane), BF16),
            pltpu.VMEM((rows_own, early, sub, lane), BF16),
        ] + [pltpu.VMEM((rows_own, size, sub, lane), BF16) for _, size in chunks] + [
            pltpu.SemaphoreType.DMA((n_k + parted - 1,)),
            pltpu.SemaphoreType.DMA((1,)),
            pltpu.SemaphoreType.DMA((2,)),
            pltpu.SemaphoreType.DMA((8,)),
            pltpu.SemaphoreType.DMA((8,)),
            pltpu.SemaphoreType.DMA((n_chunks,)),
            pltpu.SemaphoreType.DMA((n_chunks,)),
            pltpu.SemaphoreType.DMA((n_chunks,)),
            pltpu.SemaphoreType.DMA((n_chunks,)),
            pltpu.SemaphoreType.DMA((n_chunks,)),
            pltpu.SemaphoreType.DMA((2,)),
            pltpu.SemaphoreType.DMA((2,)),
        ],
        compiler_params=pltpu.CompilerParams(
            collective_id=0, has_side_effects=True, vmem_limit_bytes=54656 * 1024
        ),
        name="galerkin",
    )(a_blocks, prolong_t, packed)
    return out.astype(F32).transpose(1, 0, 2)


def solution(mesh):
    in_specs = (
        P(("grp", "dev"), None, None, None),
        P(("grp", "dev"), None, None),
        P(("grp", "dev")),
        P(),
        P(("grp", "dev"), None),
        P(("grp", "dev"), None),
        P(),
    )
    out_specs = P("dev", None, None)
    return jax.shard_map(
        functools.partial(on_device, mesh.shape["grp"], mesh.shape["dev"]),
        mesh=mesh, in_specs=in_specs, out_specs=out_specs, check_vma=False,
    )
```

```python
import functools

import jax
import jax.numpy as jnp
from jax import lax
from jax.experimental import pallas as pl
from jax.experimental.pallas import tpu as pltpu
from jax.sharding import PartitionSpec as P

EX = 4
EY = 4
MESH = pl.DeviceIdType.MESH
F32 = jnp.float32
BF16 = jnp.bfloat16


def iota(shape, dim):
    return lax.broadcasted_iota(jnp.int32, shape, dim)


def where_sum(mask, value, axis):
    return jnp.sum(jnp.where(mask, value, 0), axis=axis, keepdims=True)


def ones(mask):
    return jnp.where(mask, 1.0, 0.0).astype(BF16)


def place_of(k, n_k):
    return (k + n_k - 1) % n_k


def early_of(n_k):
    return 2


def chunks_of(n_k):
    return [(p, 2) for p in range(early_of(n_k), n_k - 1, 2)] + [(n_k - 1, 1)]


def halo_tables(grp, dev, n_grp, n_dev, halo, nbr, tab):
    device = grp * n_dev + dev
    faces, e_dev = nbr.shape
    near = [
        jnp.where(grp > 0, device - n_dev, -2),
        jnp.where(grp < n_grp - 1, device + n_dev, -2),
        jnp.where(dev > 0, device - 1, -2),
        jnp.where(dev < n_dev - 1, device + 1, -2),
    ]
    ids = nbr
    source = jnp.where(ids >= 0, jnp.maximum(ids, 0) // e_dev, -1)
    local = ids - source * e_dev
    hits = [jnp.max(jnp.where(source == n, 1.0, 0.0), axis=0, keepdims=True) for n in near]
    below = ones(iota((e_dev, e_dev), 0) < iota((e_dev, e_dev), 1))
    rank = jnp.dot(
        jnp.concatenate(hits + hits, axis=0).astype(BF16), below, preferred_element_type=F32
    ).astype(jnp.int32)
    lanes = iota((halo, e_dev), 1)
    tab[...] = jnp.zeros(tab.shape, jnp.int32)
    for d in range(4):
        found = (rank[d:d + 1] == iota((halo, e_dev), 0)) & (hits[d] > 0)
        tab[8:8 + halo, d:d + 1] = where_sum(found, lanes, 1)
    index = iota((e_dev, e_dev), 0)
    where_from = [jnp.where(source[f:f + 1] == device, local[f:f + 1], 0) for f in range(faces)]
    for d in range(4):
        seen = jnp.zeros((e_dev, e_dev), jnp.int32)
        for f in range(faces):
            seen = jnp.where(ids[f:f + 1] == near[d] * e_dev + index, 1, seen)
        seen = jnp.max(seen, axis=1, keepdims=True)
        for f in range(faces):
            ahead = where_sum(index < local[f:f + 1], seen, 0)
            where_from[f] = jnp.where(
                source[f:f + 1] == near[d], e_dev + d * halo + ahead, where_from[f]
            )
    for f in range(faces):
        tab[f:f + 1, 0:e_dev] = where_from[f]


def owner_tables(
    grp, dev, n_dev, group_rows, rows_own,
    nbr, nbr_agg, slot, touch_agg, coarse_row, tab, code, spot_of,
):
    device = grp * n_dev + dev
    faces, e_dev = nbr.shape
    touch, devices = touch_agg.shape
    lane = code.shape[1]
    groups = code.shape[0] // (faces + 1)
    rep = e_dev // groups

    def put(row, value):
        tab[row:row + 1, 0:value.shape[1]] = value

    ids = nbr
    row = iota((devices, 1), 0)
    entries = touch_agg.T
    columns = [entries[:, t:t + 1] for t in range(touch)]
    slots = slot
    own_agg = jnp.zeros((1, e_dev), jnp.int32)
    for t in range(touch):
        own_agg = jnp.where(slots == t, where_sum(row == device, columns[t], 0), own_agg)
    valid = ids >= 0
    same = valid & (nbr_agg == own_agg)
    kind = jnp.where(same, slots + touch, jnp.where(valid, slots, -1))
    kind = jnp.concatenate([slots + touch, kind], axis=0).astype(F32)
    mine = iota((groups, e_dev), 1) // rep == iota((groups, e_dev), 0)
    tall = jnp.concatenate(
        [jnp.where(mine, kind[k:k + 1], 0.0) for k in range(faces + 1)], axis=0
    ).astype(BF16)
    place = ones(iota((e_dev, lane), 0) % rep == iota((e_dev, lane), 1) // (lane // rep))
    code[...] = jnp.dot(tall, place, preferred_element_type=F32).astype(jnp.int32)

    n_agg = coarse_row.shape[1]
    numbers = coarse_row
    across = iota((devices, n_agg), 1)
    targets = [where_sum(columns[t] == across, numbers, 1) for t in range(touch)]
    owners = [target // rows_own for target in targets]
    spot = iota((devices, rows_own), 1)
    present = jnp.zeros((devices, rows_own), F32)
    for t in range(touch):
        here = jnp.where(owners[t] == dev, targets[t] - owners[t] * rows_own, -1)
        present = jnp.where(here == spot, 1.0, present)
    mates = ones(iota((devices, devices), 0) // n_dev == iota((devices, devices), 1) // n_dev)
    shared = jnp.dot(mates, present.astype(BF16), preferred_element_type=F32) > 0
    shared = jnp.where(shared, 1.0, 0.0)
    lower = ones(iota((rows_own, rows_own), 0) < iota((rows_own, rows_own), 1))
    order = jnp.dot(shared.astype(BF16), lower, preferred_element_type=F32)
    heads = where_sum(row % n_dev == 0, shared * (order + 1.0 + (row // n_dev * group_rows).astype(F32)), 0)
    tab[...] = jnp.zeros(tab.shape, jnp.int32)
    put(0, jnp.minimum(heads.astype(jnp.int32), rows_own) - 1)
    spots = jnp.sum(present * (order + 1.0), axis=1, keepdims=True).astype(jnp.int32) - 1
    spot_of[...] = jnp.broadcast_to(spots, spot_of.shape)
    peer = iota((devices, n_dev), 1) + grp * n_dev
    put(2, where_sum(peer == iota((devices, n_dev), 0), spots, 0))
    def inverse_of(which):
        inverse = jnp.full((1, n_dev), touch, jnp.int32)
        for t in range(touch):
            own = where_sum(row == which, owners[t], 0)
            inverse = jnp.where(own == iota((1, n_dev), 1), t, inverse)
        return inverse

    put(1, inverse_of(device))
    for g in range(devices // n_dev):
        put(8 + g, inverse_of(g * n_dev + dev))


def kernel(
    n_grp, n_dev, halo, group_rows, rows_own, n_agg,
    a_ref, p_ref, packed,
    out_ref,
    near_v, own_v, near, own, code,
    a_buf, p_buf, pool, tail, pack, tail_pack, tail_in, turned, left, prod, same_sum, part_t, parts, inbox, flat, spot_of, z_in, z_out, y_out, y_in, early_rows,
    *rest,
):
    *gathered, a_sem, p_sem, t_sem, h_send, h_recv, x_send, x_recv, g_send, g_recv, f_recv, z_sem, y_sem = rest
    grp = lax.axis_index("grp")
    dev = lax.axis_index("dev")
    e_dev, width_c, width_b = p_ref.shape
    n_k = a_ref.shape[1]
    touch, _, lane = same_sum.shape
    rep = lane // width_c
    sub = width_c // rep
    groups = e_dev // rep
    chunks = chunks_of(n_k)
    early = early_of(n_k)
    rest_b = width_b - lane
    parted = a_sem.shape[0] - n_k + 1

    def a_copies(k):
        count = parted if k == 0 else 1
        size = e_dev // count
        return [
            pltpu.make_async_copy(
                a_ref.at[pl.ds(q * size, size), k], a_buf.at[k, pl.ds(q * size, size)], a_sem.at[place_of(k, n_k) + q]
            )
            for q in range(count)
        ]

    faces = n_k - 1
    nbr = packed[0:faces, 0:e_dev]
    nbr_agg = packed[8:8 + faces, 0:e_dev]
    touch_agg = packed[16:16 + touch, 0:n_grp * n_dev]
    slot = packed[24:25, 0:e_dev]
    coarse_row = packed[32:33, 0:n_agg]
    p_copy = pltpu.make_async_copy(p_ref, p_buf, p_sem.at[0])
    near_copy = pltpu.make_async_copy(near_v, near, t_sem.at[0])
    own_copy = pltpu.make_async_copy(own_v, own, t_sem.at[1])
    p_copy.start()

    barrier = pltpu.get_barrier_semaphore()
    for off in range(1, n_dev):
        pl.semaphore_signal(
            barrier, inc=1, device_id=(grp, lax.rem(dev + off, n_dev)), device_id_type=MESH
        )
    for off in range(1, n_grp):
        pl.semaphore_signal(
            barrier, inc=1, device_id=(lax.rem(grp + off, n_grp), dev), device_id_type=MESH
        )

    dirs = (
        (grp > 0, (grp - 1, dev)),
        (grp < n_grp - 1, (grp + 1, dev)),
        (dev > 0, (grp, dev - 1)),
        (dev < n_dev - 1, (grp, dev + 1)),
    )

    def halo_copy(part, d, target, back):
        source, sink, base, size = ((pack, pool, e_dev, halo), (tail_pack, tail_in, 0, halo // 2))[part]
        return pltpu.make_async_remote_copy(
            src_ref=source.at[pl.ds(d * size, size)],
            dst_ref=sink.at[pl.ds(base + back * size, size)],
            send_sem=h_send.at[4 * part + d],
            recv_sem=h_recv.at[4 * part + back],
            device_id=target,
            device_id_type=MESH,
        )

    def tables_one():
        halo_tables(grp, dev, n_grp, n_dev, halo, nbr, near_v)
        near_copy.start()

    def tables_two():
        owner_tables(
            grp, dev, n_dev, group_rows, rows_own,
            nbr, nbr_agg, slot, touch_agg, coarse_row, own_v, code, spot_of,
        )
        part_t[touch] = jnp.zeros(part_t.shape[1:], BF16)
        for g in range(n_grp):
            for p in range(early):
                z_in[g, p, touch] = jnp.zeros(part_t.shape[1:], BF16)
        own_copy.start()

    def a_first():
        for copy in a_copies(1):
            copy.start()

    def p_wait():
        p_copy.wait()
        for k in list(range(2, n_k)) + [0]:
            for copy in a_copies(k):
                copy.start()

    def turn_p():
        turn = ones(
            iota((width_c, width_c), 1)
            == iota((width_c, width_c), 0) % sub * rep + iota((width_c, width_c), 0) // sub
        )

        @pl.loop(0, e_dev, unroll=e_dev)
        def _(e):
            turned[e] = jnp.dot(turn, p_buf[e], preferred_element_type=F32).astype(BF16)

    def halo_start():
        near_copy.wait()
        def start(part):
            for d, (there, target) in enumerate(dirs):
                @pl.when(there)
                def _(d=d, target=target):
                    halo_copy(part, d, target, d ^ 1).start()

        for j in range(4 * halo):
            pack[j] = p_buf[near[8 + j % halo, j // halo], :, :lane]
        pl.semaphore_wait(barrier, n_dev + n_grp - 2)
        start(0)
        for j in range(0, 4 * halo, 2):
            first = p_buf[near[8 + j % halo, j // halo], :, lane:]
            second = p_buf[near[8 + j % halo + 1, j // halo], :, lane:]
            tail_pack[j // 2] = jnp.concatenate([first, second], axis=1)
        start(1)
        pool[0:e_dev] = p_buf[:, :, :lane]
        tail[0:e_dev] = p_buf[:, :, lane:]

    def halo_wait():
        for d, (there, target) in enumerate(dirs):
            @pl.when(there)
            def _(d=d, target=target):
                for part in range(2):
                    halo_copy(part, d, target, d ^ 1).wait_send()
                    halo_copy(part, d, target, d).wait_recv()
                for j in range(d * halo // 2, (d + 1) * halo // 2):
                    both = tail_in[j]
                    tail[e_dev + 2 * j] = both[:, :rest_b]
                    tail[e_dev + 2 * j + 1] = both[:, rest_b:]

    def left_of(k, part=0, count=1):
        size = e_dev // count

        @pl.loop(part * size, (part + 1) * size, unroll=size)
        def _(e):
            rows = pl.ds(pl.multiple_of(e * width_c, width_c), width_c)
            left[k, rows, :] = jnp.dot(
                turned[e], a_buf[k, e], preferred_element_type=F32
            ).astype(BF16)

    def a_wait(*ks):
        for k in ks:
            for copy in a_copies(k):
                copy.wait()

    group_of_lane = iota((width_c, lane), 1) // width_c
    sub_lane = iota((sub, lane), 1) // width_c

    def squeeze(total):
        pieces = [total[j * sub:(j + 1) * sub] for j in range(rep)]
        out = None
        for s in range(rep):
            picked = pieces[s]
            for g in range(1, rep):
                picked = jnp.where(sub_lane == g, pieces[(g + s) % rep], picked)
            if s:
                picked = pltpu.roll(picked, s * width_c, 1)
            out = picked if out is None else out + picked
        return out

    def right_mm(k, part=0, count=1):
        size = groups // count

        @pl.loop(part * size, (part + 1) * size, unroll=size)
        def _(g):
            if k:
                at = [near[k - 1, g * rep + i] for i in range(rep)]
                blocks = [jnp.concatenate([pool[i], tail[i]], axis=1) for i in at]
            else:
                blocks = [p_buf[g * rep + i] for i in range(rep)]
            rows = pl.ds(pl.multiple_of(g * lane, lane), lane)
            full = lax.dot_general(
                left[k, rows, :], jnp.concatenate(blocks, axis=0),
                (((1,), (1,)), ((), ())), preferred_element_type=F32,
            )
            picked = full[0:width_c]
            for i in range(1, rep):
                picked = jnp.where(group_of_lane == i, full[i * width_c:(i + 1) * width_c], picked)
            prod[k, g] = picked

    def own_last():
        for q, copy in enumerate(a_copies(0)):
            copy.wait()
            left_of(0, q, parted)
            right_mm(0, q, parted)

    def right_sum(k):
        def masked(t):
            total = None
            for g in range(groups):
                at = k * groups + g
                term = jnp.where(code[at:at + 1, :] == t, prod[k, g], 0.0)
                total = term if total is None else total + term
            return total

        p = place_of(k, n_k)
        for t in range(touch):
            together = masked(t + touch)
            if k != 1:
                together = same_sum[t] + together
            if k:
                same_sum[t] = together
            value = squeeze(masked(t) if k else together).astype(BF16)
            if p < early:
                z_out[p, t] = value
                z_in[grp, p, t] = value
            else:
                part_t[t] = value
        if p >= early:
            for o in range(n_dev):
                parts[p, o] = part_t[own[1, o]]
            inbox[p, dev] = parts[p, dev]

    def column_copy(p, off):
        return pltpu.make_async_remote_copy(
            src_ref=z_out.at[p],
            dst_ref=z_in.at[grp, p, pl.ds(0, touch)],
            send_sem=z_sem.at[0],
            recv_sem=z_sem.at[1],
            device_id=(lax.rem(grp + off, n_grp), dev),
            device_id_type=MESH,
        )

    def column_all():
        others = z_in.at[pl.ds(0, n_grp - 1), :, pl.ds(0, touch)]
        return pltpu.make_async_remote_copy(
            src_ref=others,
            dst_ref=others,
            send_sem=z_sem.at[0],
            recv_sem=z_sem.at[1],
            device_id=(lax.rem(grp + 1, n_grp), dev),
            device_id_type=MESH,
        )

    def column_start(p):
        for off in range(1, n_grp):
            column_copy(p, off).start()

    def plane_copy(off):
        target = lax.rem(dev + off, n_dev)
        return pltpu.make_async_remote_copy(
            src_ref=y_out.at[target],
            dst_ref=y_in.at[dev],
            send_sem=y_sem.at[0],
            recv_sem=y_sem.at[1],
            device_id=(grp, target),
            device_id_type=MESH,
        )

    def plane_all():
        others = y_in.at[pl.ds(0, n_dev - 1)]
        return pltpu.make_async_remote_copy(
            src_ref=others,
            dst_ref=others,
            send_sem=y_sem.at[0],
            recv_sem=y_sem.at[1],
            device_id=(grp, lax.rem(dev + 1, n_dev)),
            device_id_type=MESH,
        )

    def plane_start():
        column_all().wait_recv()
        for o in range(n_dev):
            for g in range(n_grp):
                for p in range(early):
                    y_out[o, g, p] = z_in[g, p, own[8 + g, o]]
        y_in[dev] = y_out[dev]
        for off in range(1, n_dev):
            plane_copy(off).start()

    def early_place():
        plane_all().wait_recv()

        @pl.loop(0, n_grp, unroll=n_grp)
        def _(g):
            spots = [spot_of[pl.ds(g * n_dev + d, 1), :] for d in range(n_dev)]
            for p in range(early):
                values = [y_in[d, g, p].astype(F32) for d in range(n_dev)]
                for j in range(group_rows):
                    total = None
                    for d in range(n_dev):
                        term = jnp.where(spots[d] == j, values[d], 0.0)
                        total = term if total is None else total + term
                    early_rows[g * group_rows + j, p] = total.astype(BF16)

        for p in range(early):
            put_rows(early_rows, p, p + 1)

    def part_copy(c, off):
        start, size = chunks[c]
        target = lax.rem(dev + off, n_dev)
        return pltpu.make_async_remote_copy(
            src_ref=parts.at[pl.ds(start, size), target],
            dst_ref=inbox.at[pl.ds(start, size), dev],
            send_sem=x_send.at[c],
            recv_sem=x_recv.at[c],
            device_id=(grp, target),
            device_id_type=MESH,
        )

    def part_all(c):
        start, size = chunks[c]
        return pltpu.make_async_remote_copy(
            src_ref=parts.at[pl.ds(start, size), pl.ds(0, n_dev - 1)],
            dst_ref=inbox.at[pl.ds(start, size), pl.ds(0, n_dev - 1)],
            send_sem=x_send.at[c],
            recv_sem=x_recv.at[c],
            device_id=(grp, lax.rem(dev + 1, n_dev)),
            device_id_type=MESH,
        )

    def relayed(c):
        return n_grp == 4 and c < 1

    def block_of(c, sender):
        return gathered[c].at[pl.ds(sender * group_rows, group_rows)]

    def row_copy(c, sender, target, sem):
        return pltpu.make_async_remote_copy(
            src_ref=block_of(c, sender),
            dst_ref=block_of(c, sender),
            send_sem=g_send.at[c],
            recv_sem=sem,
            device_id=(target, dev),
            device_id_type=MESH,
        )

    def row_all(c, count):
        rows = gathered[c].at[pl.ds(0, count * group_rows)]
        return pltpu.make_async_remote_copy(
            src_ref=rows,
            dst_ref=rows,
            send_sem=g_send.at[c],
            recv_sem=g_recv.at[c],
            device_id=(lax.rem(grp + 1, n_grp), dev),
            device_id_type=MESH,
        )

    def send_rows(c):
        if not relayed(c):
            for off in range(1, n_grp):
                row_copy(c, grp, lax.rem(grp + off, n_grp), g_recv.at[c]).start()
            return
        for g in range(4):
            @pl.when(grp == g)
            def _(g=g):
                for target in sorted(range(4), key=lambda t: abs(t - g)):
                    if 0 < abs(target - g) < 3:
                        far = (g, target) in ((0, 2), (3, 1))
                        row_copy(c, g, target, f_recv.at[c] if far else g_recv.at[c]).start()

    def relay(c):
        for g, sender in ((1, 3), (2, 0)):
            @pl.when(grp == g)
            def _(g=g, sender=sender):
                row_copy(c, sender, g, f_recv.at[c]).wait_recv()
                row_copy(c, sender, 3 - sender, g_recv.at[c]).start()

    def rows_arrived(c):
        if not relayed(c):
            row_all(c, n_grp - 1).wait_recv()
            return
        inner = (grp == 1) | (grp == 2)

        @pl.when(inner)
        def _():
            row_all(c, 2).wait_recv()

        @pl.when(jnp.logical_not(inner))
        def _():
            row_all(c, 3).wait_recv()

    def rows_sent(c):
        if not relayed(c):
            row_all(c, n_grp - 1).wait_send()
            return
        inner = (grp == 1) | (grp == 2)

        @pl.when(inner)
        def _():
            row_all(c, 4).wait_send()

        @pl.when(jnp.logical_not(inner))
        def _():
            row_all(c, 2).wait_send()

    def exchange(c):
        for off in range(1, n_dev):
            part_copy(c, off).start()

    def collect(c):
        part_all(c).wait_recv()
        start, size = chunks[c]
        for j in range(group_rows):
            for i in range(size):
                total = jnp.zeros((sub, lane), F32)
                for d in range(n_dev):
                    member = jnp.where(own[2, d] == j, 1.0, 0.0).astype(F32)
                    total = total + inbox[start + i, d].astype(F32) * member
                gathered[c][grp * group_rows + j, i] = total.astype(BF16)
        send_rows(c)

    def put_rows(rows, i, k):
        @pl.loop(0, rows_own, unroll=8)
        def _(r):
            at = own[0, r]
            row = rows[jnp.maximum(at, 0), i].astype(F32)
            flat[pl.ds(pl.multiple_of(r * sub, sub), sub), :] = jnp.where(at >= 0, row, 0.0)

        for j in range(sub):
            out_ref[k, :, j * lane:(j + 1) * lane] = flat[pl.ds(j, rows_own, stride=sub), :].astype(BF16)

    def place(c):
        rows_arrived(c)
        start, size = chunks[c]
        for i in range(size):
            put_rows(gathered[c], i, (start + i + 1) % n_k)

    def sent():
        column_all().wait_send()
        plane_all().wait_send()
        for c in range(len(chunks)):
            part_all(c).wait_send()
            rows_sent(c)

    tables_one()
    a_first()
    tables_two()
    p_wait()
    halo_start()
    turn_p()
    a_wait(1)
    left_of(1)
    a_wait(2)
    left_of(2)
    own_copy.wait()
    a_wait(3)
    left_of(3)
    a_wait(4)
    left_of(4)
    halo_wait()
    right_mm(1)
    right_mm(2)
    right_mm(3)
    right_mm(4)
    right_sum(1)
    right_sum(2)
    right_sum(3)
    right_sum(4)
    exchange(0)
    column_start(0)
    column_start(1)
    a_wait(5,6)
    left_of(5)
    left_of(6)
    right_mm(5)
    right_mm(6)
    right_sum(5)
    right_sum(6)
    exchange(1)
    a_wait(0)
    left_of(0)
    right_mm(0)
    right_sum(0)
    exchange(2)
    collect(0)
    plane_start()
    collect(1)
    collect(2)
    relay(0)
    early_place()
    place(0)
    place(1)
    place(2)
    sent()


def on_device(n_grp, n_dev, a_blocks, prolong_t, elem_slot, touch_agg, nbr, nbr_agg, coarse_row):
    e_dev, width_c, width_b = prolong_t.shape
    n_k = a_blocks.shape[1]
    touch = touch_agg.shape[1]
    halo = e_dev // EX
    half_y = EY // 2
    span_y = half_y + 1
    group_rows = (n_dev * half_y + 1 + half_y) // span_y
    rows_own = n_grp * group_rows
    assert touch <= n_dev
    lane = 128
    rep = lane // width_c
    sub = width_c // rep
    groups = e_dev // rep
    chunks = chunks_of(n_k)
    n_chunks = len(chunks)
    early = early_of(n_k)
    parted = 1
    hbm = pl.BlockSpec(memory_space=pltpu.HBM)
    vmem = pl.BlockSpec(memory_space=pltpu.VMEM)
    ints = [nbr.T, nbr_agg.T, touch_agg.T, elem_slot.reshape(1, e_dev), coarse_row.reshape(1, -1)]
    width = -(-max(x.shape[1] for x in ints) // lane) * lane
    packed = sum(
        jnp.pad(x, ((8 * i, 8 * (len(ints) - i) - x.shape[0]), (0, width - x.shape[1])))
        for i, x in enumerate(ints)
    )
    out = pl.pallas_call(
        functools.partial(kernel, n_grp, n_dev, halo, group_rows, rows_own, coarse_row.shape[0]),
        out_shape=jax.ShapeDtypeStruct((n_k, rows_own, width_c * width_c), BF16),
        in_specs=[hbm] * 2 + [vmem],
        out_specs=vmem,
        scratch_shapes=[
            pltpu.VMEM((16, lane), jnp.int32),
            pltpu.VMEM((8 + -(-n_grp // 8) * 8, lane), jnp.int32),
            pltpu.SMEM((16, lane), jnp.int32),
            pltpu.SMEM((8 + -(-n_grp // 8) * 8, lane), jnp.int32),
            pltpu.VMEM((n_k * groups, lane), jnp.int32),
            pltpu.VMEM((n_k, e_dev, width_b, width_b), BF16),
            pltpu.VMEM((e_dev, width_c, width_b), BF16),
            pltpu.VMEM((e_dev + 4 * halo, width_c, lane), BF16),
            pltpu.VMEM((e_dev + 4 * halo, width_c, width_b - lane), BF16),
            pltpu.VMEM((4 * halo, width_c, lane), BF16),
            pltpu.VMEM((2 * halo, width_c, lane), BF16),
            pltpu.VMEM((2 * halo, width_c, lane), BF16),
            pltpu.VMEM((e_dev, width_c, width_b), BF16),
            pltpu.VMEM((n_k, e_dev * width_c, width_b), BF16),
            pltpu.VMEM((n_k, groups, width_c, lane), F32),
            pltpu.VMEM((touch, width_c, lane), F32),
            pltpu.VMEM((touch + 1, sub, lane), BF16),
            pltpu.VMEM((n_k, n_dev, sub, lane), BF16),
            pltpu.VMEM((n_k, n_dev, sub, lane), BF16),
            pltpu.VMEM((rows_own * sub, lane), F32),
            pltpu.VMEM((n_grp * n_dev, lane), jnp.int32),
            pltpu.VMEM((n_grp, early, touch + 1, sub, lane), BF16),
            pltpu.VMEM((early, touch, sub, lane), BF16),
            pltpu.VMEM((n_dev, n_grp, early, sub, lane), BF16),
            pltpu.VMEM((n_dev, n_grp, early, sub, lane), BF16),
            pltpu.VMEM((rows_own, early, sub, lane), BF16),
        ] + [pltpu.VMEM((rows_own, size, sub, lane), BF16) for _, size in chunks] + [
            pltpu.SemaphoreType.DMA((n_k + parted - 1,)),
            pltpu.SemaphoreType.DMA((1,)),
            pltpu.SemaphoreType.DMA((2,)),
            pltpu.SemaphoreType.DMA((8,)),
            pltpu.SemaphoreType.DMA((8,)),
            pltpu.SemaphoreType.DMA((n_chunks,)),
            pltpu.SemaphoreType.DMA((n_chunks,)),
            pltpu.SemaphoreType.DMA((n_chunks,)),
            pltpu.SemaphoreType.DMA((n_chunks,)),
            pltpu.SemaphoreType.DMA((n_chunks,)),
            pltpu.SemaphoreType.DMA((2,)),
            pltpu.SemaphoreType.DMA((2,)),
        ],
        compiler_params=pltpu.CompilerParams(
            collective_id=0, has_side_effects=True, vmem_limit_bytes=54656 * 1024
        ),
        name="galerkin",
    )(a_blocks, prolong_t, packed)
    return out.astype(F32).transpose(1, 0, 2)


def solution(mesh):
    in_specs = (
        P(("grp", "dev"), None, None, None),
        P(("grp", "dev"), None, None),
        P(("grp", "dev")),
        P(),
        P(("grp", "dev"), None),
        P(("grp", "dev"), None),
        P(),
    )
    out_specs = P("dev", None, None)
    return jax.shard_map(
        functools.partial(on_device, mesh.shape["grp"], mesh.shape["dev"]),
        mesh=mesh, in_specs=in_specs, out_specs=out_specs, check_vma=False,
    )
```
